16 devices in a mesh: dp: 2 (over y, z), tp: 8 (over x, core).
Axes of the slice: x: 4, y: 2, z: 1, core: 2. Of those that a mesh axis runs over, the one named last changes fastest.
The devices are a block of a 4x4x8 slice.
Arguments:
- x: bfloat16 [256, 4096], P('dp'), parts along dimension 0
- ln_attn_gamma: float32 [4096], replicated
- ln_attn_beta: float32 [4096], replicated
- ln_mlp_gamma: float32 [4096], replicated
- ln_mlp_beta: float32 [4096], replicated
- w_qkv: bfloat16 [4096, 32, 3, 128], P(None, 'tp')
- w_out: bfloat16 [32, 1, 128, 4096], P('tp')
- w_up: bfloat16 [4096, 16384], P(None, 'tp')
- w_down: bfloat16 [16384, 4096], P('tp')
- k_cache: bfloat16 [256, 32, 128, 128], P('dp', 'tp'), parts along dimension 0
- v_cache: bfloat16 [256, 32, 128, 128], P('dp', 'tp'), parts along dimension 0
- positions: int32 [256], P('dp'), parts along dimension 0
Outputs:
- output 1: bfloat16 [256, 4096], P('dp'), parts along dimension 0
- output 2: bfloat16 [256, 32, 128, 128], P('dp', 'tp'), parts along dimension 0
- output 3: bfloat16 [256, 32, 128, 128], P('dp', 'tp'), parts along dimension 0
There are 2 independent parts. The reference program is written for one: setup_inputs(seed, part) draws one part's arguments, and reference() takes and returns one part's arrays. A program takes and returns all parts, laid end to end along the dimension named above; an argument that names none is the same for every part.
All inputs are finite; a program needn't handle non-finite values.
Results may differ from the reference program's by a relative error of at most 0.0118648.
Values are sent between devices in bfloat16 or wider.
A program may use at most 768 MiB of HBM per device.

```python
import math
import jax
import jax.numpy as jnp
from jax import lax

D = 4096
GROUPS = 32
QPG = 1
HEAD = 128
FF = 16384
BATCH = 128
SEQ = 128

QKV_SLOTS = QPG + 2
HALF_HEAD = HEAD // 2
SCORE_SCALE = 1.0 / math.sqrt(HEAD)
LN_EPS = 1e-5
ROPE_BASE = 10000.0
NEG_BIG = -1e30


def setup_inputs(seed: int = 0, part: int = 0) -> dict:
    shared_key, part_base = jax.random.split(jax.random.key(seed))
    shared = jax.random.split(shared_key, 8)
    local = jax.random.split(jax.random.fold_in(part_base, part), 8)
    x = jax.random.normal(local[0], (BATCH, D), jnp.float32).astype(jnp.bfloat16)
    ln_attn_gamma = 1.0 + 0.3 * jax.random.normal(shared[0], (D,), jnp.float32)
    ln_attn_beta = 0.3 * jax.random.normal(shared[1], (D,), jnp.float32)
    ln_mlp_gamma = 1.0 + 0.3 * jax.random.normal(shared[2], (D,), jnp.float32)
    ln_mlp_beta = 0.3 * jax.random.normal(shared[3], (D,), jnp.float32)
    w_qkv = (jax.random.normal(shared[4], (D, GROUPS, QKV_SLOTS, HEAD), jnp.float32) * D ** -0.5).astype(jnp.bfloat16)
    w_out = (jax.random.normal(shared[5], (GROUPS, QPG, HEAD, D), jnp.float32) * (GROUPS * QPG * HEAD) ** -0.5).astype(jnp.bfloat16)
    w_up = (jax.random.normal(shared[6], (D, FF), jnp.float32) * D ** -0.5).astype(jnp.bfloat16)
    w_down = (jax.random.normal(shared[7], (FF, D), jnp.float32) * FF ** -0.5).astype(jnp.bfloat16)
    ramp = (2.0 * jnp.arange(SEQ, dtype=jnp.float32) / SEQ - 1.0)[None, None, :, None]
    k_slope = 1.5 * jax.random.normal(local[1], (BATCH, GROUPS, 1, HEAD), jnp.float32)
    k_cache = (jax.random.normal(local[2], (BATCH, GROUPS, SEQ, HEAD), jnp.float32) + ramp * k_slope).astype(jnp.bfloat16)
    v_level = jax.random.normal(local[3], (BATCH, GROUPS, 1, HEAD), jnp.float32)
    v_slope = jax.random.normal(local[4], (BATCH, GROUPS, 1, HEAD), jnp.float32)
    v_cache = (0.5 * jax.random.normal(local[5], (BATCH, GROUPS, SEQ, HEAD), jnp.float32) + v_level + ramp * v_slope).astype(jnp.bfloat16)
    positions = jax.random.randint(local[6], (BATCH,), SEQ // 4, SEQ, dtype=jnp.int32)
    positions = positions.at[0].set(SEQ - 1).at[1].set(SEQ // 4)
    return {'x': x, 'ln_attn_gamma': ln_attn_gamma, 'ln_attn_beta': ln_attn_beta, 'ln_mlp_gamma': ln_mlp_gamma, 'ln_mlp_beta': ln_mlp_beta, 'w_qkv': w_qkv, 'w_out': w_out, 'w_up': w_up, 'w_down': w_down, 'k_cache': k_cache, 'v_cache': v_cache, 'positions': positions}


def layer_norm(act_rows, ln_gamma, ln_beta):
    rows_f32 = act_rows.astype(jnp.float32)
    row_mean = jnp.mean(rows_f32, axis=-1, keepdims=True)
    centred = rows_f32 - row_mean
    row_var = jnp.mean(centred * centred, axis=-1, keepdims=True)
    return (centred * lax.rsqrt(row_var + LN_EPS) * ln_gamma + ln_beta).astype(jnp.bfloat16)


def apply_rotary(vectors, cos_t, sin_t):
    as_f32 = vectors.astype(jnp.float32)
    lower_half = as_f32[..., :HALF_HEAD]
    upper_half = as_f32[..., HALF_HEAD:]
    return jnp.concatenate([lower_half * cos_t - upper_half * sin_t, upper_half * cos_t + lower_half * sin_t], axis=-1).astype(jnp.bfloat16)


def reference(x, ln_attn_gamma, ln_attn_beta, ln_mlp_gamma, ln_mlp_beta, w_qkv, w_out, w_up, w_down, k_cache, v_cache, positions):
    attn_in = layer_norm(x, ln_attn_gamma, ln_attn_beta)
    mlp_in = layer_norm(x, ln_mlp_gamma, ln_mlp_beta)
    qkv_rows = jnp.dot(attn_in, w_qkv.reshape(D, GROUPS * QKV_SLOTS * HEAD), preferred_element_type=jnp.float32).astype(jnp.bfloat16)
    qkv_rows = qkv_rows.reshape(BATCH, GROUPS, QKV_SLOTS, HEAD)
    inv_freq = ROPE_BASE ** (-2.0 * jnp.arange(HALF_HEAD, dtype=jnp.float32) / HEAD)
    angles = positions.astype(jnp.float32)[:, None] * inv_freq[None, :]
    cos_t = jnp.cos(angles)
    sin_t = jnp.sin(angles)
    queries = apply_rotary(qkv_rows[:, :, :QPG], cos_t[:, None, None, :], sin_t[:, None, None, :])
    new_key = apply_rotary(qkv_rows[:, :, QPG], cos_t[:, None, :], sin_t[:, None, :])
    new_value = qkv_rows[:, :, QPG + 1]
    slot_ids = jnp.arange(SEQ)
    write_mask = (slot_ids[None, :] == positions[:, None])[:, None, :, None]
    keys_all = jnp.where(write_mask, new_key[:, :, None, :], k_cache)
    values_all = jnp.where(write_mask, new_value[:, :, None, :], v_cache)
    valid_mask = slot_ids[None, :] <= positions[:, None]

    def attend_group(operands):
        q_grp, k_grp, v_grp = operands
        scores = jnp.einsum('bqh,bsh->bqs', q_grp.astype(jnp.float32), k_grp.astype(jnp.float32)) * SCORE_SCALE
        scores = jnp.where(valid_mask[:, None, :], scores, NEG_BIG)
        attn_probs = jax.nn.softmax(scores, axis=-1).astype(jnp.bfloat16)
        return jnp.einsum('bqs,bsh->bqh', attn_probs.astype(jnp.float32), v_grp.astype(jnp.float32)).astype(jnp.bfloat16)

    context = lax.map(attend_group, (jnp.moveaxis(queries, 1, 0), jnp.moveaxis(keys_all, 1, 0), jnp.moveaxis(values_all, 1, 0)))
    context = jnp.moveaxis(context, 0, 1).reshape(BATCH, GROUPS * QPG * HEAD)
    attn_out = jnp.dot(context, w_out.reshape(GROUPS * QPG * HEAD, D), preferred_element_type=jnp.float32)
    hidden = jax.nn.gelu(jnp.dot(mlp_in, w_up, preferred_element_type=jnp.float32), approximate=False).astype(jnp.bfloat16)
    mlp_out = jnp.dot(hidden, w_down, preferred_element_type=jnp.float32)
    layer_out = (x.astype(jnp.float32) + attn_out + mlp_out).astype(jnp.bfloat16)
    return (layer_out, keys_all, values_all)
```

```python
import functools

import jax
import jax.numpy as jnp
from jax import lax
from jax.experimental import pallas as pl
from jax.experimental.pallas import tpu as pltpu
from jax.sharding import PartitionSpec as P

LN_EPS = 1e-5
ROPE_BASE = 10000.0
NEG_BIG = -1e30
LANES = 128
ROWS_PER_CHUNK = 8
W_CHUNK = 256
F32 = jnp.float32
BF16 = jnp.bfloat16
ANY = pl.BlockSpec(memory_space=pl.ANY)
VMEM = pl.BlockSpec(memory_space=pltpu.VMEM)
SMEM = pl.BlockSpec(memory_space=pltpu.SMEM)


def norm_into(x_ref, gamma_ref, beta_ref, dst_ref):
    rows, width = x_ref.shape
    tiles = width // LANES

    def tile(c):
        return x_ref[:, pl.ds(pl.multiple_of(c * LANES, LANES), LANES)].astype(F32)

    zero = jnp.zeros((rows, LANES), F32)
    total = lax.fori_loop(0, tiles, lambda c, s: s + tile(c), zero, unroll=4)
    mean = jnp.sum(total, axis=-1, keepdims=True) / width

    def square(c, s):
        d = tile(c) - mean
        return s + d * d

    var = jnp.sum(lax.fori_loop(0, tiles, square, zero, unroll=4), axis=-1, keepdims=True) / width
    inv = lax.rsqrt(var + LN_EPS)

    def write(c, carry):
        y = (tile(c) - mean) * inv * gamma_ref[pl.ds(c, 1), :] + beta_ref[pl.ds(c, 1), :]
        dst_ref[:, pl.ds(pl.multiple_of(c * LANES, LANES), LANES)] = y.astype(BF16)
        return carry

    lax.fori_loop(0, tiles, write, 0, unroll=4)


def attention_kernel(pos_ref, x_ref, gamma_ref, beta_ref, cos_ref, sin_ref, w_ref, k_ref, v_ref, ctx_ref, ko_ref, vo_ref,
                     wbuf, wf, acc, attn, q_s, kn_s, vn_s, kbuf, vbuf, wsem, insem, outsem):
    rows, width = x_ref.shape
    _, groups, slots, head = k_ref.shape
    cols = 3 * groups
    n_w = width // W_CHUNK
    n_c = rows // ROWS_PER_CHUNK
    wrows = W_CHUNK * cols

    def w_copy(c):
        at = pl.ds(pl.multiple_of(c * wrows, wrows), wrows)
        return pltpu.make_async_copy(w_ref.at[at], wbuf.at[at], wsem.at[c])

    def io(i, which, out):
        hbm_in, hbm_out, buf = ((k_ref, ko_ref, kbuf), (v_ref, vo_ref, vbuf))[which]
        at = pl.ds(i * ROWS_PER_CHUNK, ROWS_PER_CHUNK)
        if out:
            return pltpu.make_async_copy(buf.at[at], hbm_out.at[at], outsem.at[which, i])
        return pltpu.make_async_copy(hbm_in.at[at], buf.at[at], insem.at[which, i])

    for c in range(n_w):
        w_copy(c).start()
    for i in range(n_c):
        io(i, 0, False).start()
        io(i, 1, False).start()

    norm_into(x_ref, gamma_ref, beta_ref, attn)
    acc[...] = jnp.zeros_like(acc)

    def project(c, carry):
        w_copy(c).wait()
        wf[...] = wbuf[pl.ds(pl.multiple_of(c * wrows, wrows), wrows), :].astype(F32)
        lhs = attn[:, pl.ds(pl.multiple_of(c * W_CHUNK, W_CHUNK), W_CHUNK)]
        for n in range(0, cols, 2):
            rhs = jnp.concatenate(
                [wf[pl.ds(n + e, W_CHUNK, stride=cols), :].astype(BF16) for e in range(2)], axis=1)
            acc[:, n * head:(n + 2) * head] += jnp.dot(lhs, rhs, preferred_element_type=F32)
        return carry

    lax.fori_loop(0, n_w, project, 0)

    cos_t, sin_t = cos_ref[...], sin_ref[...]

    def rotate(u):
        u = u.astype(BF16).astype(F32)
        return (u * cos_t + pltpu.roll(u, head // 2, 1) * sin_t).astype(BF16).astype(F32)

    for g in range(groups):
        at = pl.ds(g, rows, stride=groups)
        q_s[at, :] = rotate(acc[:, g * head:(g + 1) * head])
        kn_s[at, :] = rotate(acc[:, (groups + g) * head:(groups + g + 1) * head])
        vn_s[at, :] = acc[:, (2 * groups + g) * head:(2 * groups + g + 1) * head].astype(BF16).astype(F32)

    row16 = lax.broadcasted_iota(jnp.int32, (16, head), 0)
    row8 = lax.broadcasted_iota(jnp.int32, (2 * groups, slots), 0)
    lane8 = lax.broadcasted_iota(jnp.int32, (2 * groups, slots), 1)
    scale = head ** -0.5

    def chunk(i, carry):
        io(i, 0, False).wait()
        io(i, 1, False).wait()

        def write_row(r, carry):
            b = i * ROWS_PER_CHUNK + r
            pos = pos_ref[b]
            base = pl.multiple_of((pos // 16) * 16, 16)
            hit = row16 == pos - base
            for g in range(groups):
                for buf, new in ((kbuf, kn_s), (vbuf, vn_s)):
                    old = buf[b, g, pl.ds(base, 16), :].astype(F32)
                    row = new[pl.ds(b * groups + g, 1), :]
                    buf[b, g, pl.ds(base, 16), :] = jnp.where(hit, row, old).astype(BF16)
            return carry

        lax.fori_loop(0, ROWS_PER_CHUNK, write_row, 0, unroll=True)
        io(i, 0, True).start()
        io(i, 1, True).start()

        for pair in range(ROWS_PER_CHUNK // 2):
            b = i * ROWS_PER_CHUNK + 2 * pair
            at = pl.ds(pl.multiple_of(b * groups, 2 * groups), 2 * groups)
            q8 = q_s[at, :].astype(BF16)
            keys = kbuf[pl.ds(b, 2)].reshape(2 * groups * slots, head)
            every = lax.dot_general(q8, keys, (((1,), (1,)), ((), ())), preferred_element_type=F32)
            s = every[:, 0:slots]
            for t in range(1, 2 * groups):
                s = jnp.where(row8 == t, every[:, t * slots:(t + 1) * slots], s)
            pos8 = jnp.where(row8 < groups, pos_ref[b], pos_ref[b + 1])
            s = jnp.where(lane8 <= pos8, s * scale, NEG_BIG)
            e = jnp.exp(s - jnp.max(s, axis=-1, keepdims=True))
            p = e / jnp.sum(e, axis=-1, keepdims=True)
            spread = jnp.concatenate([jnp.where(row8 == t, p, 0.0) for t in range(2 * groups)], axis=1).astype(BF16)
            values = vbuf[pl.ds(b, 2)].reshape(2 * groups * slots, head)
            ctx_ref[at, :] = jnp.dot(spread, values, preferred_element_type=F32).astype(BF16).astype(F32)
        return carry

    lax.fori_loop(0, n_c, chunk, 0)
    for i in range(n_c):
        io(i, 0, True).wait()
        io(i, 1, True).wait()


def attend(x, gamma, beta, w_qkv, k_cache, v_cache, positions):
    rows, width = x.shape
    _, groups, slots, head = k_cache.shape
    cols = 3 * groups
    inv_freq = ROPE_BASE ** (-2.0 * jnp.arange(head // 2, dtype=F32) / head)
    angles = positions.astype(F32)[:, None] * inv_freq[None, :]
    cos_t, sin_t = jnp.cos(angles), jnp.sin(angles)
    cos_t = jnp.concatenate([cos_t, cos_t], axis=1)
    sin_t = jnp.concatenate([-sin_t, sin_t], axis=1)
    w_rows = jnp.transpose(w_qkv, (0, 2, 1, 3)).reshape(width * cols, head)
    n_w, n_c = width // W_CHUNK, rows // ROWS_PER_CHUNK
    return pl.pallas_call(
        attention_kernel,
        out_shape=[jax.ShapeDtypeStruct((rows * groups, head), F32),
                   jax.ShapeDtypeStruct(k_cache.shape, k_cache.dtype),
                   jax.ShapeDtypeStruct(v_cache.shape, v_cache.dtype)],
        in_specs=[SMEM, VMEM, VMEM, VMEM, VMEM, VMEM, ANY, ANY, ANY],
        out_specs=[VMEM, ANY, ANY],
        scratch_shapes=[
            pltpu.VMEM((width * cols, head), BF16),
            pltpu.VMEM((W_CHUNK * cols, head), F32),
            pltpu.VMEM((rows, cols * head), F32),
            pltpu.VMEM((rows, width), BF16),
            pltpu.VMEM((rows * groups, head), F32),
            pltpu.VMEM((rows * groups, head), F32),
            pltpu.VMEM((rows * groups, head), F32),
            pltpu.VMEM(k_cache.shape, BF16),
            pltpu.VMEM(v_cache.shape, BF16),
            pltpu.SemaphoreType.DMA((n_w,)),
            pltpu.SemaphoreType.DMA((2, n_c)),
            pltpu.SemaphoreType.DMA((2, n_c)),
        ],
        compiler_params=pltpu.CompilerParams(vmem_limit_bytes=60 * 1024 * 1024),
        name='attend',
    )(positions, x, gamma.reshape(-1, LANES), beta.reshape(-1, LANES), cos_t, sin_t, w_rows, k_cache, v_cache)


def layer_norm(act_rows, ln_gamma, ln_beta):
    rows_f32 = act_rows.astype(jnp.float32)
    row_mean = jnp.mean(rows_f32, axis=-1, keepdims=True)
    centred = rows_f32 - row_mean
    row_var = jnp.mean(centred * centred, axis=-1, keepdims=True)
    return (centred * lax.rsqrt(row_var + LN_EPS) * ln_gamma + ln_beta).astype(jnp.bfloat16)


def solution(mesh):
    row_spec = P('dp', None)
    vec_spec = P(None)
    cache_spec = P('dp', 'tp', None, None)

    def device_step(x, ln_attn_gamma, ln_attn_beta, ln_mlp_gamma, ln_mlp_beta, w_qkv, w_out, w_up, w_down, k_cache, v_cache, positions):
        mlp_in = layer_norm(x, ln_mlp_gamma, ln_mlp_beta)
        context, keys_all, values_all = attend(x, ln_attn_gamma, ln_attn_beta, w_qkv, k_cache, v_cache, positions)
        rows = x.shape[0]
        context = context.astype(BF16).reshape(rows, -1)
        attn_part = jnp.dot(context, w_out.reshape(-1, x.shape[1]), preferred_element_type=jnp.float32)
        hidden = jax.nn.gelu(jnp.dot(mlp_in, w_up, preferred_element_type=jnp.float32), approximate=False).astype(jnp.bfloat16)
        mlp_part = jnp.dot(hidden, w_down, preferred_element_type=jnp.float32)
        total = lax.psum((attn_part + mlp_part).astype(BF16), 'tp')
        layer_out = (x.astype(jnp.float32) + total.astype(jnp.float32)).astype(jnp.bfloat16)
        return layer_out, keys_all, values_all

    return jax.shard_map(device_step, mesh=mesh, in_specs=(row_spec, vec_spec, vec_spec, vec_spec, vec_spec, P(None, 'tp', None, None), P('tp', None, None, None), P(None, 'tp'), P('tp', None), cache_spec, cache_spec, P('dp')), out_specs=(row_spec, cache_spec, cache_spec), check_vma=False)
```

```python
import jax
import jax.numpy as jnp
from jax import lax
from jax.experimental import pallas as pl
from jax.experimental.pallas import tpu as pltpu
from jax.sharding import PartitionSpec as P

LN_EPS = 1e-5
ROPE_BASE = 10000.0
NEG_BIG = -1e30
LANES = 128
ROWS_PER_CHUNK = 8
W_CHUNK = 256
UP_COLS = 512
OUT_COLS = 512
F32 = jnp.float32
BF16 = jnp.bfloat16
ANY = pl.BlockSpec(memory_space=pl.ANY)
VMEM = pl.BlockSpec(memory_space=pltpu.VMEM)
SMEM = pl.BlockSpec(memory_space=pltpu.SMEM)
MESH = pl.DeviceIdType.MESH


def norm_into(x_ref, gamma_ref, beta_ref, dst_ref):
    rows, width = x_ref.shape
    tiles = width // LANES

    def tile(c):
        return x_ref[:, pl.ds(pl.multiple_of(c * LANES, LANES), LANES)].astype(F32)

    zero = jnp.zeros((rows, LANES), F32)
    total = lax.fori_loop(0, tiles, lambda c, s: s + tile(c), zero, unroll=4)
    mean = jnp.sum(total, axis=-1, keepdims=True) / width

    def square(c, s):
        d = tile(c) - mean
        return s + d * d

    var = jnp.sum(lax.fori_loop(0, tiles, square, zero, unroll=4), axis=-1, keepdims=True) / width
    inv = lax.rsqrt(var + LN_EPS)

    def write(c, carry):
        y = (tile(c) - mean) * inv * gamma_ref[pl.ds(c, 1), :] + beta_ref[pl.ds(c, 1), :]
        dst_ref[:, pl.ds(pl.multiple_of(c * LANES, LANES), LANES)] = y.astype(BF16)
        return carry

    lax.fori_loop(0, tiles, write, 0, unroll=4)


def attention_kernel(pos_ref, x_ref, gamma_ref, beta_ref, cos_ref, sin_ref, w_ref, k_ref, v_ref, ctx_ref, ko_ref, vo_ref,
                     wbuf, wf, acc, attn, q_s, kn_s, vn_s, kbuf, vbuf, wsem, insem, outsem):
    rows, width = x_ref.shape
    _, groups, slots, head = k_ref.shape
    cols = 3 * groups
    n_w = width // W_CHUNK
    n_c = rows // ROWS_PER_CHUNK
    wrows = W_CHUNK * cols

    def w_copy(c):
        at = pl.ds(pl.multiple_of(c * wrows, wrows), wrows)
        return pltpu.make_async_copy(w_ref.at[at], wbuf.at[at], wsem.at[c])

    def io(i, which, out):
        hbm_in, hbm_out, buf = ((k_ref, ko_ref, kbuf), (v_ref, vo_ref, vbuf))[which]
        at = pl.ds(i * ROWS_PER_CHUNK, ROWS_PER_CHUNK)
        if out:
            return pltpu.make_async_copy(buf.at[at], hbm_out.at[at], outsem.at[which, i])
        return pltpu.make_async_copy(hbm_in.at[at], buf.at[at], insem.at[which, i])

    for c in range(n_w):
        w_copy(c).start()
    for i in range(n_c):
        io(i, 0, False).start()
        io(i, 1, False).start()

    norm_into(x_ref, gamma_ref, beta_ref, attn)
    acc[...] = jnp.zeros_like(acc)

    def project(c, carry):
        w_copy(c).wait()
        wf[...] = wbuf[pl.ds(pl.multiple_of(c * wrows, wrows), wrows), :].astype(F32)
        lhs = attn[:, pl.ds(pl.multiple_of(c * W_CHUNK, W_CHUNK), W_CHUNK)]
        for n in range(0, cols, 2):
            rhs = jnp.concatenate(
                [wf[pl.ds(n + e, W_CHUNK, stride=cols), :].astype(BF16) for e in range(2)], axis=1)
            acc[:, n * head:(n + 2) * head] += jnp.dot(lhs, rhs, preferred_element_type=F32)
        return carry

    lax.fori_loop(0, n_w, project, 0)

    cos_t, sin_t = cos_ref[...], sin_ref[...]

    def rotate(u):
        u = u.astype(BF16).astype(F32)
        return (u * cos_t + pltpu.roll(u, head // 2, 1) * sin_t).astype(BF16).astype(F32)

    for g in range(groups):
        at = pl.ds(g, rows, stride=groups)
        q_s[at, :] = rotate(acc[:, g * head:(g + 1) * head])
        kn_s[at, :] = rotate(acc[:, (groups + g) * head:(groups + g + 1) * head])
        vn_s[at, :] = acc[:, (2 * groups + g) * head:(2 * groups + g + 1) * head].astype(BF16).astype(F32)

    row16 = lax.broadcasted_iota(jnp.int32, (16, head), 0)
    row8 = lax.broadcasted_iota(jnp.int32, (2 * groups, slots), 0)
    lane8 = lax.broadcasted_iota(jnp.int32, (2 * groups, slots), 1)
    scale = head ** -0.5

    def chunk(i, carry):
        io(i, 0, False).wait()
        io(i, 1, False).wait()

        def write_row(r, carry):
            b = i * ROWS_PER_CHUNK + r
            pos = pos_ref[b]
            base = pl.multiple_of((pos // 16) * 16, 16)
            hit = row16 == pos - base
            for g in range(groups):
                for buf, new in ((kbuf, kn_s), (vbuf, vn_s)):
                    old = buf[b, g, pl.ds(base, 16), :].astype(F32)
                    row = new[pl.ds(b * groups + g, 1), :]
                    buf[b, g, pl.ds(base, 16), :] = jnp.where(hit, row, old).astype(BF16)
            return carry

        lax.fori_loop(0, ROWS_PER_CHUNK, write_row, 0, unroll=True)
        io(i, 0, True).start()
        io(i, 1, True).start()

        for pair in range(ROWS_PER_CHUNK // 2):
            b = i * ROWS_PER_CHUNK + 2 * pair
            at = pl.ds(pl.multiple_of(b * groups, 2 * groups), 2 * groups)
            q8 = q_s[at, :].astype(BF16)
            keys = kbuf[pl.ds(b, 2)].reshape(2 * groups * slots, head)
            every = lax.dot_general(q8, keys, (((1,), (1,)), ((), ())), preferred_element_type=F32)
            s = every[:, 0:slots]
            for t in range(1, 2 * groups):
                s = jnp.where(row8 == t, every[:, t * slots:(t + 1) * slots], s)
            pos8 = jnp.where(row8 < groups, pos_ref[b], pos_ref[b + 1])
            s = jnp.where(lane8 <= pos8, s * scale, NEG_BIG)
            e = jnp.exp(s - jnp.max(s, axis=-1, keepdims=True))
            p = e / jnp.sum(e, axis=-1, keepdims=True)
            spread = jnp.concatenate([jnp.where(row8 == t, p, 0.0) for t in range(2 * groups)], axis=1).astype(BF16)
            values = vbuf[pl.ds(b, 2)].reshape(2 * groups * slots, head)
            ctx_ref[at, :] = jnp.dot(spread, values, preferred_element_type=F32).astype(BF16).astype(F32)
        return carry

    lax.fori_loop(0, n_c, chunk, 0)
    for i in range(n_c):
        io(i, 0, True).wait()
        io(i, 1, True).wait()


def attend(x, gamma, beta, w_qkv, k_cache, v_cache, positions):
    rows, width = x.shape
    _, groups, slots, head = k_cache.shape
    cols = 3 * groups
    inv_freq = ROPE_BASE ** (-2.0 * jnp.arange(head // 2, dtype=F32) / head)
    angles = positions.astype(F32)[:, None] * inv_freq[None, :]
    cos_t, sin_t = jnp.cos(angles), jnp.sin(angles)
    cos_t = jnp.concatenate([cos_t, cos_t], axis=1)
    sin_t = jnp.concatenate([-sin_t, sin_t], axis=1)
    w_rows = jnp.transpose(w_qkv, (0, 2, 1, 3)).reshape(width * cols, head)
    n_w, n_c = width // W_CHUNK, rows // ROWS_PER_CHUNK
    return pl.pallas_call(
        attention_kernel,
        out_shape=[jax.ShapeDtypeStruct((rows * groups, head), F32),
                   jax.ShapeDtypeStruct(k_cache.shape, k_cache.dtype),
                   jax.ShapeDtypeStruct(v_cache.shape, v_cache.dtype)],
        in_specs=[SMEM, VMEM, VMEM, VMEM, VMEM, VMEM, ANY, ANY, ANY],
        out_specs=[VMEM, ANY, ANY],
        scratch_shapes=[
            pltpu.VMEM((width * cols, head), BF16),
            pltpu.VMEM((W_CHUNK * cols, head), F32),
            pltpu.VMEM((rows, cols * head), F32),
            pltpu.VMEM((rows, width), BF16),
            pltpu.VMEM((rows * groups, head), F32),
            pltpu.VMEM((rows * groups, head), F32),
            pltpu.VMEM((rows * groups, head), F32),
            pltpu.VMEM(k_cache.shape, BF16),
            pltpu.VMEM(v_cache.shape, BF16),
            pltpu.SemaphoreType.DMA((n_w,)),
            pltpu.SemaphoreType.DMA((2, n_c)),
            pltpu.SemaphoreType.DMA((2, n_c)),
        ],
        compiler_params=pltpu.CompilerParams(vmem_limit_bytes=60 * 1024 * 1024),
        name='attend',
    )(positions, x, gamma.reshape(-1, LANES), beta.reshape(-1, LANES), cos_t, sin_t, w_rows, k_cache, v_cache)


def mlp_kernel(x_ref, gamma_ref, beta_ref, ctx_ref, wo_ref, wu_ref, wd_ref, out_ref,
               wub, wdb, wob, mlp_in, hid, ctxb, part, d2d_src, d2d_dst, cs32, csb, relay_a, relay_b, comb_a, comb_b,
               from_l, from_r, outb, usem, dsem, osem, send, recv, stored):
    n_u, _, cu = wub.shape
    n_b, _, cb = wdb.shape
    half, slab = d2d_src.shape[1], relay_a.shape[1]
    chips = half // slab
    groups = ctxb.shape[1] // LANES
    rows = x_ref.shape[0]
    me = lax.axis_index('tp')
    p, c = lax.div(me, 2), lax.rem(me, 2)
    right = 2 * lax.rem(p + 1, chips) + c
    left = 2 * lax.rem(p + chips - 1, chips) + c
    partner = me + 1 - 2 * c
    lo, hi = pl.ds(0, cb // 2), pl.ds(cb // 2, cb // 2)

    def up_copy(u):
        return pltpu.make_async_copy(wu_ref.at[:, pl.ds(u * cu, cu)], wub.at[u], usem.at[u])

    def down_copy(j):
        return pltpu.make_async_copy(wd_ref.at[:, pl.ds(j * cb, cb)], wdb.at[j], dsem.at[j])

    def out_copy(j):
        return pltpu.make_async_copy(wo_ref.at[:, pl.ds(j * cb, cb)], wob.at[j], osem.at[j])

    for u in range(n_u):
        up_copy(u).start()
    for j in range(n_b):
        out_copy(j).start()
        down_copy(j).start()

    barrier = pltpu.get_barrier_semaphore()
    for peer in (right, left, partner):
        pl.semaphore_signal(barrier, inc=1, device_id={'tp': peer}, device_id_type=MESH)

    def in_half(q):
        return pl.ds(pl.multiple_of(lax.rem(p + q, chips) * slab, slab), slab)

    def in_rows(q, core):
        return pl.ds(pl.multiple_of(core * half + lax.rem(p + q, chips) * slab, slab), slab)

    def remote(kind, j):
        mine, before, after, far = (in_rows(q, c) for q in (0, chips - 1, 1, 2))
        src, dst, peer = (
            (d2d_src.at[j], d2d_dst.at[j], partner),
            (csb.at[j, in_half(2), lo], relay_a.at[j], right),
            (csb.at[j, in_half(2), hi], relay_b.at[j], left),
            (csb.at[j, in_half(1), hi], from_l.at[j, :, hi], right),
            (csb.at[j, in_half(chips - 1), lo], from_r.at[j, :, lo], left),
            (comb_a.at[j], from_l.at[j, :, lo], right),
            (comb_b.at[j], from_r.at[j, :, hi], left),
            (outb.at[j, mine], outb.at[j, mine], right),
            (outb.at[j, mine], outb.at[j, mine], left),
            (outb.at[j, mine], outb.at[j, mine], partner),
            (outb.at[j, before, lo], outb.at[j, before, lo], right),
            (outb.at[j, after, hi], outb.at[j, after, hi], left),
            (outb.at[j, before], outb.at[j, before], partner),
            (outb.at[j, after], outb.at[j, after], partner),
            (outb.at[j, far], outb.at[j, far], partner),
        )[kind]
        return pltpu.make_async_remote_copy(src_ref=src, dst_ref=dst, send_sem=send.at[kind, j], recv_sem=recv.at[kind, j],
                                            device_id={'tp': peer}, device_id_type=MESH)

    norm_into(x_ref, gamma_ref, beta_ref, mlp_in)
    for g in range(groups):
        ctxb[:, g * LANES:(g + 1) * LANES] = ctx_ref[pl.ds(g, rows, stride=groups), :].astype(BF16)

    def up(u, carry):
        up_copy(u).wait()
        z = jnp.dot(mlp_in[...], wub[u], preferred_element_type=F32)
        hid[u] = (0.5 * z * (1.0 + lax.erf(z * 0.5 ** 0.5))).astype(BF16)
        return carry

    lax.fori_loop(0, n_u, up, 0)
    pl.semaphore_wait(barrier, 3)

    own_half = pl.ds(pl.multiple_of(c * half, half), half)
    other_half = pl.ds(pl.multiple_of((1 - c) * half, half), half)

    def compute(j):
        out_copy(j).wait()
        y = jnp.dot(ctxb[...], wob[j], preferred_element_type=F32)
        down_copy(j).wait()
        for u in range(n_u):
            y += jnp.dot(hid[u], wdb[j, u * cu:(u + 1) * cu, :], preferred_element_type=F32)
        part[j] = y
        d2d_src[j] = part[j, other_half].astype(BF16)
        remote(0, j).start()

    def chip_sum(j):
        remote(0, j).wait_recv()
        y = part[j, own_half] + d2d_dst[j].astype(F32)
        cs32[j] = y
        csb[j] = y.astype(BF16)
        for kind in (1, 2, 3, 4):
            remote(kind, j).start()

    def combine(j):
        remote(1, j).wait_recv()
        comb_a[j] = (cs32[j, in_half(1), lo] + relay_a[j].astype(F32)).astype(BF16)
        remote(5, j).start()
        remote(2, j).wait_recv()
        comb_b[j] = (cs32[j, in_half(chips - 1), hi] + relay_b[j].astype(F32)).astype(BF16)
        remote(6, j).start()

    def finish(j):
        for kind in (3, 4, 5, 6):
            remote(kind, j).wait_recv()
        mine = in_rows(0, c)
        y = cs32[j, in_half(0)] + from_l[j].astype(F32) + from_r[j].astype(F32)
        outb[j, mine] = (x_ref[mine, j * cb:(j + 1) * cb].astype(F32) + y).astype(BF16)
        for kind in (7, 8, 9):
            remote(kind, j).start()

    def forward(j):
        remote(7, j).wait_recv()
        remote(10, j).start()
        remote(12, j).start()
        remote(8, j).wait_recv()
        remote(11, j).start()
        remote(13, j).start()

    def share(j):
        remote(10, j).wait_recv()
        remote(11, j).wait_recv()
        remote(14, j).start()

    def store(j):
        return pltpu.make_async_copy(outb.at[j], out_ref.at[:, pl.ds(j * cb, cb)], stored.at[j])

    def collect(j):
        for kind in (9, 12, 13, 14):
            remote(kind, j).wait_recv()
        store(j).start()

    stages = ((compute, 0), (chip_sum, 1), (combine, 3), (finish, 5), (forward, 7), (share, 9), (collect, 10))
    for step in range(n_b + stages[-1][1]):
        for stage, lag in stages:
            if 0 <= step - lag < n_b:
                stage(step - lag)
    for j in range(n_b):
        for kind in range(15):
            remote(kind, j).wait_send()
        store(j).wait()


def mlp_and_sum(mesh, x, gamma, beta, context, w_out, w_up, w_down):
    rows, width = x.shape
    hidden = w_up.shape[1]
    ctx_width = w_out.shape[0]
    chips = mesh.shape['tp'] // 2
    assert chips == 4
    n_u, n_b = hidden // UP_COLS, width // OUT_COLS
    half, slab = rows // 2, rows // 2 // chips

    def block(dtype, *shape):
        return pltpu.VMEM((n_b,) + shape, dtype)

    return pl.pallas_call(
        mlp_kernel,
        out_shape=jax.ShapeDtypeStruct(x.shape, x.dtype),
        in_specs=[VMEM, VMEM, VMEM, VMEM, ANY, ANY, ANY],
        out_specs=ANY,
        scratch_shapes=[
            pltpu.VMEM((n_u, width, UP_COLS), BF16),
            block(BF16, hidden, OUT_COLS),
            block(BF16, ctx_width, OUT_COLS),
            pltpu.VMEM((rows, width), BF16),
            pltpu.VMEM((n_u, rows, UP_COLS), BF16),
            pltpu.VMEM((rows, ctx_width), BF16),
            block(F32, rows, OUT_COLS),
            block(BF16, half, OUT_COLS),
            block(BF16, half, OUT_COLS),
            block(F32, half, OUT_COLS),
            block(BF16, half, OUT_COLS),
            block(BF16, slab, OUT_COLS // 2),
            block(BF16, slab, OUT_COLS // 2),
            block(BF16, slab, OUT_COLS // 2),
            block(BF16, slab, OUT_COLS // 2),
            block(BF16, slab, OUT_COLS),
            block(BF16, slab, OUT_COLS),
            block(BF16, rows, OUT_COLS),
            pltpu.SemaphoreType.DMA((n_u,)),
            pltpu.SemaphoreType.DMA((n_b,)),
            pltpu.SemaphoreType.DMA((n_b,)),
            pltpu.SemaphoreType.DMA((15, n_b)),
            pltpu.SemaphoreType.DMA((15, n_b)),
            pltpu.SemaphoreType.DMA((n_b,)),
        ],
        compiler_params=pltpu.CompilerParams(vmem_limit_bytes=60 * 1024 * 1024, collective_id=0, has_side_effects=True),
        name='mlp_and_sum',
    )(x, gamma.reshape(-1, LANES), beta.reshape(-1, LANES), context, w_out, w_up, w_down)


def solution(mesh):
    row_spec = P('dp', None)
    vec_spec = P(None)
    cache_spec = P('dp', 'tp', None, None)

    def device_step(x, ln_attn_gamma, ln_attn_beta, ln_mlp_gamma, ln_mlp_beta, w_qkv, w_out, w_up, w_down, k_cache, v_cache, positions):
        context, keys_all, values_all = attend(x, ln_attn_gamma, ln_attn_beta, w_qkv, k_cache, v_cache, positions)
        layer_out = mlp_and_sum(mesh, x, ln_mlp_gamma, ln_mlp_beta, context, w_out.reshape(-1, x.shape[1]), w_up, w_down)
        return layer_out, keys_all, values_all

    return jax.shard_map(device_step, mesh=mesh, in_specs=(row_spec, vec_spec, vec_spec, vec_spec, vec_spec, P(None, 'tp', None, None), P('tp', None, None, None), P(None, 'tp'), P('tp', None), cache_spec, cache_spec, P('dp')), out_specs=(row_spec, cache_spec, cache_spec), check_vma=False)
```

```python
import jax
import jax.numpy as jnp
from jax import lax
from jax.experimental import pallas as pl
from jax.experimental.pallas import tpu as pltpu
from jax.sharding import PartitionSpec as P

LN_EPS = 1e-5
ROPE_BASE = 10000.0
NEG_BIG = -1e30
LANES = 128
ROWS_PER_CHUNK = 8
W_CHUNK = 256
UP_COLS = 512
OUT_COLS = 512
F32 = jnp.float32
BF16 = jnp.bfloat16
ANY = pl.BlockSpec(memory_space=pl.ANY)
VMEM = pl.BlockSpec(memory_space=pltpu.VMEM)
SMEM = pl.BlockSpec(memory_space=pltpu.SMEM)
MESH = pl.DeviceIdType.MESH


def norm_into(x_ref, gamma_ref, beta_ref, dst_ref):
    rows, width = x_ref.shape
    tiles = width // LANES

    def tile(c):
        return x_ref[:, pl.ds(pl.multiple_of(c * LANES, LANES), LANES)].astype(F32)

    zero = jnp.zeros((rows, LANES), F32)
    total = lax.fori_loop(0, tiles, lambda c, s: s + tile(c), zero, unroll=4)
    mean = jnp.sum(total, axis=-1, keepdims=True) / width

    def square(c, s):
        d = tile(c) - mean
        return s + d * d

    var = jnp.sum(lax.fori_loop(0, tiles, square, zero, unroll=4), axis=-1, keepdims=True) / width
    inv = lax.rsqrt(var + LN_EPS)

    def write(c, carry):
        y = (tile(c) - mean) * inv * gamma_ref[pl.ds(c, 1), :] + beta_ref[pl.ds(c, 1), :]
        dst_ref[:, pl.ds(pl.multiple_of(c * LANES, LANES), LANES)] = y.astype(BF16)
        return carry

    lax.fori_loop(0, tiles, write, 0, unroll=4)


def attention_kernel(pos_ref, x_ref, gamma_ref, beta_ref, cos_ref, sin_ref, w_ref, k_ref, v_ref, ctx_ref, ko_ref, vo_ref,
                     wbuf, wf, acc, attn, q_s, kn_s, vn_s, kbuf, vbuf, wsem, insem, outsem):
    rows, width = x_ref.shape
    _, groups, slots, head = k_ref.shape
    cols = 3 * groups
    n_w = width // W_CHUNK
    n_c = rows // ROWS_PER_CHUNK
    wrows = W_CHUNK * cols

    def w_copy(c):
        at = pl.ds(pl.multiple_of(c * wrows, wrows), wrows)
        return pltpu.make_async_copy(w_ref.at[at], wbuf.at[at], wsem.at[c])

    def io(i, which, out):
        hbm_in, hbm_out, buf = ((k_ref, ko_ref, kbuf), (v_ref, vo_ref, vbuf))[which]
        at = pl.ds(i * ROWS_PER_CHUNK, ROWS_PER_CHUNK)
        if out:
            return pltpu.make_async_copy(buf.at[at], hbm_out.at[at], outsem.at[which, i])
        return pltpu.make_async_copy(hbm_in.at[at], buf.at[at], insem.at[which, i])

    for c in range(n_w):
        w_copy(c).start()
    for i in range(n_c):
        io(i, 0, False).start()
        io(i, 1, False).start()

    norm_into(x_ref, gamma_ref, beta_ref, attn)
    acc[...] = jnp.zeros_like(acc)

    def project(c, carry):
        w_copy(c).wait()
        wf[...] = wbuf[pl.ds(pl.multiple_of(c * wrows, wrows), wrows), :].astype(F32)
        lhs = attn[:, pl.ds(pl.multiple_of(c * W_CHUNK, W_CHUNK), W_CHUNK)]
        for n in range(0, cols, 2):
            rhs = jnp.concatenate(
                [wf[pl.ds(n + e, W_CHUNK, stride=cols), :].astype(BF16) for e in range(2)], axis=1)
            acc[:, n * head:(n + 2) * head] += jnp.dot(lhs, rhs, preferred_element_type=F32)
        return carry

    lax.fori_loop(0, n_w, project, 0)

    cos_t, sin_t = cos_ref[...], sin_ref[...]

    def rotate(u):
        u = u.astype(BF16).astype(F32)
        return (u * cos_t + pltpu.roll(u, head // 2, 1) * sin_t).astype(BF16).astype(F32)

    for g in range(groups):
        at = pl.ds(g, rows, stride=groups)
        q_s[at, :] = rotate(acc[:, g * head:(g + 1) * head])
        kn_s[at, :] = rotate(acc[:, (groups + g) * head:(groups + g + 1) * head])
        vn_s[at, :] = acc[:, (2 * groups + g) * head:(2 * groups + g + 1) * head].astype(BF16).astype(F32)

    row16 = lax.broadcasted_iota(jnp.int32, (16, head), 0)
    per_chunk = ROWS_PER_CHUNK * groups
    slot_id = lax.broadcasted_iota(jnp.int32, (slots, per_chunk), 0)
    lane_id = lax.broadcasted_iota(jnp.int32, (slots, per_chunk), 1)
    scale = head ** -0.5

    def chunk(i, carry):
        io(i, 0, False).wait()
        io(i, 1, False).wait()

        def write_row(r, carry):
            b = i * ROWS_PER_CHUNK + r
            pos = pos_ref[b]
            base = pl.multiple_of((pos // 16) * 16, 16)
            hit = row16 == pos - base
            for g in range(groups):
                for buf, new in ((kbuf, kn_s), (vbuf, vn_s)):
                    old = buf[b, g, pl.ds(base, 16), :].astype(F32)
                    row = new[pl.ds(b * groups + g, 1), :]
                    buf[b, g, pl.ds(base, 16), :] = jnp.where(hit, row, old).astype(BF16)
            return carry

        lax.fori_loop(0, ROWS_PER_CHUNK, write_row, 0, unroll=True)
        io(i, 0, True).start()
        io(i, 1, True).start()

        at = pl.ds(pl.multiple_of(i * per_chunk, per_chunk), per_chunk)
        queries = q_s[at, :].astype(BF16)
        s = jnp.zeros((slots, per_chunk), F32)
        limit = jnp.zeros((slots, per_chunk), jnp.int32)
        for r in range(ROWS_PER_CHUNK):
            b = i * ROWS_PER_CHUNK + r
            every = lax.dot_general(kbuf[b].reshape(groups * slots, head), queries, (((1,), (1,)), ((), ())),
                                    preferred_element_type=F32)
            for g in range(groups):
                s = jnp.where(lane_id == r * groups + g, every[g * slots:(g + 1) * slots], s)
            limit = jnp.where(lane_id >= r * groups, pos_ref[b], limit)
        s = jnp.where(slot_id <= limit, s * scale, NEG_BIG)
        e = jnp.exp(s - jnp.max(s, axis=0, keepdims=True))
        p = (e / jnp.sum(e, axis=0, keepdims=True)).astype(BF16).astype(F32)
        for r in range(ROWS_PER_CHUNK):
            b = i * ROWS_PER_CHUNK + r
            for g in range(groups):
                n = r * groups + g
                weighted = jnp.broadcast_to(p[:, n:n + 1], (slots, head)) * vbuf[b, g].astype(F32)
                ctx_ref[pl.ds(b * groups + g, 1), :] = jnp.sum(weighted, axis=0, keepdims=True).astype(BF16).astype(F32)
        return carry

    lax.fori_loop(0, n_c, chunk, 0)
    for i in range(n_c):
        io(i, 0, True).wait()
        io(i, 1, True).wait()


def attend(x, gamma, beta, w_qkv, k_cache, v_cache, positions):
    rows, width = x.shape
    _, groups, slots, head = k_cache.shape
    cols = 3 * groups
    inv_freq = ROPE_BASE ** (-2.0 * jnp.arange(head // 2, dtype=F32) / head)
    angles = positions.astype(F32)[:, None] * inv_freq[None, :]
    cos_t, sin_t = jnp.cos(angles), jnp.sin(angles)
    cos_t = jnp.concatenate([cos_t, cos_t], axis=1)
    sin_t = jnp.concatenate([-sin_t, sin_t], axis=1)
    w_rows = jnp.transpose(w_qkv, (0, 2, 1, 3)).reshape(width * cols, head)
    n_w, n_c = width // W_CHUNK, rows // ROWS_PER_CHUNK
    return pl.pallas_call(
        attention_kernel,
        out_shape=[jax.ShapeDtypeStruct((rows * groups, head), F32),
                   jax.ShapeDtypeStruct(k_cache.shape, k_cache.dtype),
                   jax.ShapeDtypeStruct(v_cache.shape, v_cache.dtype)],
        in_specs=[SMEM, VMEM, VMEM, VMEM, VMEM, VMEM, ANY, ANY, ANY],
        out_specs=[VMEM, ANY, ANY],
        scratch_shapes=[
            pltpu.VMEM((width * cols, head), BF16),
            pltpu.VMEM((W_CHUNK * cols, head), F32),
            pltpu.VMEM((rows, cols * head), F32),
            pltpu.VMEM((rows, width), BF16),
            pltpu.VMEM((rows * groups, head), F32),
            pltpu.VMEM((rows * groups, head), F32),
            pltpu.VMEM((rows * groups, head), F32),
            pltpu.VMEM(k_cache.shape, BF16),
            pltpu.VMEM(v_cache.shape, BF16),
            pltpu.SemaphoreType.DMA((n_w,)),
            pltpu.SemaphoreType.DMA((2, n_c)),
            pltpu.SemaphoreType.DMA((2, n_c)),
        ],
        compiler_params=pltpu.CompilerParams(vmem_limit_bytes=60 * 1024 * 1024),
        name='attend',
    )(positions, x, gamma.reshape(-1, LANES), beta.reshape(-1, LANES), cos_t, sin_t, w_rows, k_cache, v_cache)


def mlp_kernel(x_ref, gamma_ref, beta_ref, ctx_ref, wo_ref, wu_ref, wd_ref, out_ref,
               wub, wcat, mlp_in, lhs, part, d2d_src, d2d_dst, cs32, csb, relay_a, relay_b, comb_a, comb_b,
               from_l, from_r, outb, usem, dsem, osem, send, recv, stored):
    n_u, _, cu = wub.shape
    n_b, _, cb = wcat.shape
    half, slab = d2d_src.shape[1], relay_a.shape[1]
    chips = half // slab
    rows = x_ref.shape[0]
    ctx_width = wo_ref.shape[0]
    groups = ctx_width // LANES
    me = lax.axis_index('tp')
    p, c = lax.div(me, 2), lax.rem(me, 2)
    right = 2 * lax.rem(p + 1, chips) + c
    left = 2 * lax.rem(p + chips - 1, chips) + c
    partner = me + 1 - 2 * c
    lo, hi = pl.ds(0, cb // 2), pl.ds(cb // 2, cb // 2)

    def up_copy(u):
        return pltpu.make_async_copy(wu_ref.at[:, pl.ds(u * cu, cu)], wub.at[u], usem.at[u])

    def down_copy(j):
        return pltpu.make_async_copy(wd_ref.at[:, pl.ds(j * cb, cb)], wcat.at[j, pl.ds(ctx_width, wd_ref.shape[0])], dsem.at[j])

    def out_copy(j):
        return pltpu.make_async_copy(wo_ref.at[:, pl.ds(j * cb, cb)], wcat.at[j, pl.ds(0, ctx_width)], osem.at[j])

    for u in range(n_u):
        up_copy(u).start()
    for j in range(n_b):
        out_copy(j).start()
        down_copy(j).start()

    barrier = pltpu.get_barrier_semaphore()
    for peer in (right, left, partner):
        pl.semaphore_signal(barrier, inc=1, device_id={'tp': peer}, device_id_type=MESH)

    def in_half(q):
        return pl.ds(pl.multiple_of(lax.rem(p + q, chips) * slab, slab), slab)

    def in_rows(q, core):
        return pl.ds(pl.multiple_of(core * half + lax.rem(p + q, chips) * slab, slab), slab)

    def remote(kind, j):
        mine, before, after, far = (in_rows(q, c) for q in (0, chips - 1, 1, 2))
        src, dst, peer = (
            (d2d_src.at[j], d2d_dst.at[j], partner),
            (csb.at[j, in_half(2), lo], relay_a.at[j], right),
            (csb.at[j, in_half(2), hi], relay_b.at[j], left),
            (csb.at[j, in_half(1), hi], from_l.at[j, :, hi], right),
            (csb.at[j, in_half(chips - 1), lo], from_r.at[j, :, lo], left),
            (comb_a.at[j], from_l.at[j, :, lo], right),
            (comb_b.at[j], from_r.at[j, :, hi], left),
            (outb.at[j, mine], outb.at[j, mine], right),
            (outb.at[j, mine], outb.at[j, mine], left),
            (outb.at[j, mine], outb.at[j, mine], partner),
            (outb.at[j, before, lo], outb.at[j, before, lo], right),
            (outb.at[j, after, hi], outb.at[j, after, hi], left),
            (outb.at[j, before], outb.at[j, before], partner),
            (outb.at[j, after], outb.at[j, after], partner),
            (outb.at[j, far], outb.at[j, far], partner),
        )[kind]
        return pltpu.make_async_remote_copy(src_ref=src, dst_ref=dst, send_sem=send.at[kind, j], recv_sem=recv.at[kind, j],
                                            device_id={'tp': peer}, device_id_type=MESH)

    norm_into(x_ref, gamma_ref, beta_ref, mlp_in)
    for g in range(groups):
        lhs[:, g * LANES:(g + 1) * LANES] = ctx_ref[pl.ds(g, rows, stride=groups), :].astype(BF16)

    def up(u, carry):
        up_copy(u).wait()
        z = jnp.dot(mlp_in[...], wub[u], preferred_element_type=F32)
        lhs[:, pl.ds(pl.multiple_of(ctx_width + u * cu, cu), cu)] = (0.5 * z * (1.0 + lax.erf(z * 0.5 ** 0.5))).astype(BF16)
        return carry

    lax.fori_loop(0, n_u, up, 0)
    pl.semaphore_wait(barrier, 3)

    own_half = pl.ds(pl.multiple_of(c * half, half), half)
    other_half = pl.ds(pl.multiple_of((1 - c) * half, half), half)

    def compute(j):
        out_copy(j).wait()
        down_copy(j).wait()
        part[j] = jnp.dot(lhs[...], wcat[j], preferred_element_type=F32)
        d2d_src[j] = part[j, other_half].astype(BF16)
        remote(0, j).start()

    def chip_sum(j):
        remote(0, j).wait_recv()
        y = part[j, own_half] + d2d_dst[j].astype(F32)
        cs32[j] = y
        csb[j] = y.astype(BF16)
        for kind in (1, 2, 3, 4):
            remote(kind, j).start()

    def combine(j):
        remote(1, j).wait_recv()
        comb_a[j] = (cs32[j, in_half(1), lo] + relay_a[j].astype(F32)).astype(BF16)
        remote(5, j).start()
        remote(2, j).wait_recv()
        comb_b[j] = (cs32[j, in_half(chips - 1), hi] + relay_b[j].astype(F32)).astype(BF16)
        remote(6, j).start()

    def finish(j):
        for kind in (3, 4, 5, 6):
            remote(kind, j).wait_recv()
        mine = in_rows(0, c)
        y = cs32[j, in_half(0)] + from_l[j].astype(F32) + from_r[j].astype(F32)
        outb[j, mine] = (x_ref[mine, j * cb:(j + 1) * cb].astype(F32) + y).astype(BF16)
        for kind in (7, 8, 9):
            remote(kind, j).start()

    def forward(j):
        remote(7, j).wait_recv()
        remote(10, j).start()
        remote(12, j).start()
        remote(8, j).wait_recv()
        remote(11, j).start()
        remote(13, j).start()

    def share(j):
        remote(10, j).wait_recv()
        remote(11, j).wait_recv()
        remote(14, j).start()

    def store(j):
        return pltpu.make_async_copy(outb.at[j], out_ref.at[:, pl.ds(j * cb, cb)], stored.at[j])

    def collect(j):
        for kind in (9, 12, 13, 14):
            remote(kind, j).wait_recv()
        store(j).start()

    stages = ((compute, 0), (chip_sum, 1), (combine, 3), (finish, 5), (forward, 7), (share, 9), (collect, 10))
    for step in range(n_b + stages[-1][1]):
        for stage, lag in stages:
            if 0 <= step - lag < n_b:
                stage(step - lag)
    for j in range(n_b):
        for kind in range(15):
            remote(kind, j).wait_send()
        store(j).wait()


def mlp_and_sum(mesh, x, gamma, beta, context, w_out, w_up, w_down):
    rows, width = x.shape
    hidden = w_up.shape[1]
    ctx_width = w_out.shape[0]
    chips = mesh.shape['tp'] // 2
    assert chips == 4
    n_u, n_b = hidden // UP_COLS, width // OUT_COLS
    half, slab = rows // 2, rows // 2 // chips

    def block(dtype, *shape):
        return pltpu.VMEM((n_b,) + shape, dtype)

    return pl.pallas_call(
        mlp_kernel,
        out_shape=jax.ShapeDtypeStruct(x.shape, x.dtype),
        in_specs=[VMEM, VMEM, VMEM, VMEM, ANY, ANY, ANY],
        out_specs=ANY,
        scratch_shapes=[
            pltpu.VMEM((n_u, width, UP_COLS), BF16),
            block(BF16, ctx_width + hidden, OUT_COLS),
            pltpu.VMEM((rows, width), BF16),
            pltpu.VMEM((rows, ctx_width + hidden), BF16),
            block(F32, rows, OUT_COLS),
            block(BF16, half, OUT_COLS),
            block(BF16, half, OUT_COLS),
            block(F32, half, OUT_COLS),
            block(BF16, half, OUT_COLS),
            block(BF16, slab, OUT_COLS // 2),
            block(BF16, slab, OUT_COLS // 2),
            block(BF16, slab, OUT_COLS // 2),
            block(BF16, slab, OUT_COLS // 2),
            block(BF16, slab, OUT_COLS),
            block(BF16, slab, OUT_COLS),
            block(BF16, rows, OUT_COLS),
            pltpu.SemaphoreType.DMA((n_u,)),
            pltpu.SemaphoreType.DMA((n_b,)),
            pltpu.SemaphoreType.DMA((n_b,)),
            pltpu.SemaphoreType.DMA((15, n_b)),
            pltpu.SemaphoreType.DMA((15, n_b)),
            pltpu.SemaphoreType.DMA((n_b,)),
        ],
        compiler_params=pltpu.CompilerParams(vmem_limit_bytes=60 * 1024 * 1024, collective_id=0, has_side_effects=True),
        name='mlp_and_sum',
    )(x, gamma.reshape(-1, LANES), beta.reshape(-1, LANES), context, w_out, w_up, w_down)


def solution(mesh):
    row_spec = P('dp', None)
    vec_spec = P(None)
    cache_spec = P('dp', 'tp', None, None)

    def device_step(x, ln_attn_gamma, ln_attn_beta, ln_mlp_gamma, ln_mlp_beta, w_qkv, w_out, w_up, w_down, k_cache, v_cache, positions):
        context, keys_all, values_all = attend(x, ln_attn_gamma, ln_attn_beta, w_qkv, k_cache, v_cache, positions)
        layer_out = mlp_and_sum(mesh, x, ln_mlp_gamma, ln_mlp_beta, context, w_out.reshape(-1, x.shape[1]), w_up, w_down)
        return layer_out, keys_all, values_all

    return jax.shard_map(device_step, mesh=mesh, in_specs=(row_spec, vec_spec, vec_spec, vec_spec, vec_spec, P(None, 'tp', None, None), P('tp', None, None, None), P(None, 'tp'), P('tp', None), cache_spec, cache_spec, P('dp')), out_specs=(row_spec, cache_spec, cache_spec), check_vma=False)
```

```python
import math

import jax
import jax.numpy as jnp
from jax import lax
from jax.experimental import pallas as pl
from jax.experimental.pallas import tpu as pltpu
from jax.sharding import PartitionSpec as P

LN_EPS = 1e-5
ROPE_BASE = 10000.0
NEG_BIG = -1e30
LANES = 128
ROWS_PER_CHUNK = 8
W_CHUNK = 256
W_AHEAD = 8
KV_AHEAD = 6
UP_COLS = 256
AHEAD = 4
OUT_COLS = 512
BLOCK_US = 0.9
F32 = jnp.float32
BF16 = jnp.bfloat16
HBM = pl.BlockSpec(memory_space=pltpu.HBM)
MESH = pl.DeviceIdType.MESH


def norm_into(x_ref, gamma_ref, beta_ref, dst_ref):
    rows, width = x_ref.shape
    tiles = width // LANES

    def tile(c):
        return x_ref[:, pl.ds(pl.multiple_of(c * LANES, LANES), LANES)].astype(F32)

    zero = jnp.zeros((rows, LANES), F32)
    total = lax.fori_loop(0, tiles, lambda c, s: s + tile(c), zero, unroll=4)
    mean = jnp.sum(total, axis=-1, keepdims=True) / width

    def square(c, s):
        d = tile(c) - mean
        return s + d * d

    var = jnp.sum(lax.fori_loop(0, tiles, square, zero, unroll=4), axis=-1, keepdims=True) / width
    inv = lax.rsqrt(var + LN_EPS)

    def write(c, carry):
        y = (tile(c) - mean) * inv * gamma_ref[pl.ds(c, 1), :] + beta_ref[pl.ds(c, 1), :]
        dst_ref[:, pl.ds(pl.multiple_of(c * LANES, LANES), LANES)] = y.astype(BF16)
        return carry

    lax.fori_loop(0, tiles, write, 0, unroll=4)


def attention_kernel(pos_hbm, pos_row_hbm, x_hbm, gamma_hbm, beta_hbm, w_ref, k_ref, v_ref, ctx_hbm, ko_ref, vo_ref,
                     pos_ref, pos_row, x_ref, gamma_ref, beta_ref, ctx_ref,
                     wbuf, wf, acc, attn, q_s, kn_s, vn_s, kbuf, vbuf, small, wsem, insem, outsem):
    rows, width = x_ref.shape
    _, groups, slots, head = k_ref.shape
    cols = 3 * groups
    n_w = width // W_CHUNK
    n_c = rows // ROWS_PER_CHUNK
    wrows = W_CHUNK * cols

    def w_copy(c):
        at = pl.ds(pl.multiple_of(c * wrows, wrows), wrows)
        return pltpu.make_async_copy(w_ref.at[at], wbuf.at[at], wsem.at[c])

    def io(i, which, out):
        hbm_in, hbm_out, buf = ((k_ref, ko_ref, kbuf), (v_ref, vo_ref, vbuf))[which]
        at = pl.ds(i * ROWS_PER_CHUNK, ROWS_PER_CHUNK)
        if out:
            return pltpu.make_async_copy(buf.at[at], hbm_out.at[at], outsem.at[which, i])
        return pltpu.make_async_copy(hbm_in.at[at], buf.at[at], insem.at[which, i])

    def kv_start(i):
        io(i, 0, False).start()
        io(i, 1, False).start()

    first = [pltpu.make_async_copy(src, dst, small.at[n]) for n, (src, dst) in enumerate(
        ((x_hbm, x_ref), (gamma_hbm, gamma_ref), (beta_hbm, beta_ref), (pos_row_hbm, pos_row), (pos_hbm, pos_ref)))]
    for copy in first:
        copy.start()
    for c in range(W_AHEAD):
        w_copy(c).start()
    for copy in first:
        copy.wait()

    norm_into(x_ref, gamma_ref, beta_ref, attn)
    acc[...] = jnp.zeros_like(acc)

    def project(c, carry):
        w_copy(c).wait()

        @pl.when(c + W_AHEAD < n_w)
        def _():
            w_copy(c + W_AHEAD).start()

        @pl.when(c >= n_w - KV_AHEAD)
        def _():
            kv_start(c - (n_w - KV_AHEAD))

        wf[...] = wbuf[pl.ds(pl.multiple_of(c * wrows, wrows), wrows), :].astype(F32)
        lhs = attn[:, pl.ds(pl.multiple_of(c * W_CHUNK, W_CHUNK), W_CHUNK)]
        for n in range(0, cols, 2):
            rhs = jnp.concatenate(
                [wf[pl.ds(n + e, W_CHUNK, stride=cols), :].astype(BF16) for e in range(2)], axis=1)
            acc[:, n * head:(n + 2) * head] += jnp.dot(lhs, rhs, preferred_element_type=F32)
        return carry

    lax.fori_loop(0, n_w, project, 0)

    lane = lax.broadcasted_iota(jnp.int32, (rows, head), 1)
    freq = jnp.exp(lax.rem(lane, head // 2).astype(F32) * (-2.0 * math.log(ROPE_BASE) / head))
    angle = jnp.broadcast_to(pos_row[...].astype(F32), (rows, rows)).T * freq
    cos_t = jnp.cos(angle)
    sin_t = jnp.where(lane < head // 2, -1.0, 1.0) * jnp.sin(angle)

    def rotate(u):
        u = u.astype(BF16).astype(F32)
        return (u * cos_t + pltpu.roll(u, head // 2, 1) * sin_t).astype(BF16).astype(F32)

    for g in range(groups):
        at = pl.ds(g, rows, stride=groups)
        q_s[at, :] = rotate(acc[:, g * head:(g + 1) * head])
        kn_s[at, :] = rotate(acc[:, (groups + g) * head:(groups + g + 1) * head])
        vn_s[at, :] = acc[:, (2 * groups + g) * head:(2 * groups + g + 1) * head].astype(BF16).astype(F32)

    row16 = lax.broadcasted_iota(jnp.int32, (16, head), 0)
    per_chunk = ROWS_PER_CHUNK * groups
    slot_id = lax.broadcasted_iota(jnp.int32, (slots, per_chunk), 0)
    lane_id = lax.broadcasted_iota(jnp.int32, (slots, per_chunk), 1)
    scale = head ** -0.5

    def chunk(i, carry):
        io(i, 0, False).wait()
        io(i, 1, False).wait()

        @pl.when(i + KV_AHEAD < n_c)
        def _():
            kv_start(i + KV_AHEAD)

        def write_row(r, carry):
            b = i * ROWS_PER_CHUNK + r
            pos = pos_ref[b]
            base = pl.multiple_of((pos // 16) * 16, 16)
            hit = row16 == pos - base
            for g in range(groups):
                for buf, new in ((kbuf, kn_s), (vbuf, vn_s)):
                    old = buf[b, g, pl.ds(base, 16), :].astype(F32)
                    row = new[pl.ds(b * groups + g, 1), :]
                    buf[b, g, pl.ds(base, 16), :] = jnp.where(hit, row, old).astype(BF16)
            return carry

        lax.fori_loop(0, ROWS_PER_CHUNK, write_row, 0, unroll=True)
        io(i, 0, True).start()
        io(i, 1, True).start()

        at = pl.ds(pl.multiple_of(i * per_chunk, per_chunk), per_chunk)
        queries = q_s[at, :].astype(BF16)
        s = jnp.zeros((slots, per_chunk), F32)
        limit = jnp.zeros((slots, per_chunk), jnp.int32)
        for r in range(ROWS_PER_CHUNK):
            b = i * ROWS_PER_CHUNK + r
            every = lax.dot_general(kbuf[b].reshape(groups * slots, head), queries, (((1,), (1,)), ((), ())),
                                    preferred_element_type=F32)
            for g in range(groups):
                s = jnp.where(lane_id == r * groups + g, every[g * slots:(g + 1) * slots], s)
            limit = jnp.where(lane_id >= r * groups, pos_ref[b], limit)
        s = jnp.where(slot_id <= limit, s * scale, NEG_BIG)
        e = jnp.exp(s - jnp.max(s, axis=0, keepdims=True))
        p = (e / jnp.sum(e, axis=0, keepdims=True)).astype(BF16).astype(F32)
        for r in range(ROWS_PER_CHUNK):
            b = i * ROWS_PER_CHUNK + r
            for g in range(groups):
                n = r * groups + g
                weighted = jnp.broadcast_to(p[:, n:n + 1], (slots, head)) * vbuf[b, g].astype(F32)
                ctx_ref[pl.ds(b * groups + g, 1), :] = jnp.sum(weighted, axis=0, keepdims=True).astype(BF16).astype(F32)
        return carry

    lax.fori_loop(0, n_c, chunk, 0)
    ctx_out = pltpu.make_async_copy(ctx_ref, ctx_hbm, small.at[0])
    ctx_out.start()
    for i in range(n_c):
        io(i, 0, True).wait()
        io(i, 1, True).wait()
    ctx_out.wait()


def attend(x, gamma, beta, w_qkv, k_cache, v_cache, positions):
    rows, width = x.shape
    _, groups, slots, head = k_cache.shape
    cols = 3 * groups
    w_rows = jnp.transpose(w_qkv, (0, 2, 1, 3)).reshape(width * cols, head)
    n_w, n_c = width // W_CHUNK, rows // ROWS_PER_CHUNK
    return pl.pallas_call(
        attention_kernel,
        out_shape=[jax.ShapeDtypeStruct((rows * groups, head), F32),
                   jax.ShapeDtypeStruct(k_cache.shape, k_cache.dtype),
                   jax.ShapeDtypeStruct(v_cache.shape, v_cache.dtype)],
        in_specs=[HBM] * 8,
        out_specs=[HBM] * 3,
        scratch_shapes=[
            pltpu.SMEM((rows,), jnp.int32),
            pltpu.VMEM((1, rows), jnp.int32),
            pltpu.VMEM((rows, width), BF16),
            pltpu.VMEM((width // LANES, LANES), F32),
            pltpu.VMEM((width // LANES, LANES), F32),
            pltpu.VMEM((rows * groups, head), F32),
            pltpu.VMEM((width * cols, head), BF16),
            pltpu.VMEM((W_CHUNK * cols, head), F32),
            pltpu.VMEM((rows, cols * head), F32),
            pltpu.VMEM((rows, width), BF16),
            pltpu.VMEM((rows * groups, head), F32),
            pltpu.VMEM((rows * groups, head), F32),
            pltpu.VMEM((rows * groups, head), F32),
            pltpu.VMEM(k_cache.shape, BF16),
            pltpu.VMEM(v_cache.shape, BF16),
            pltpu.SemaphoreType.DMA((5,)),
            pltpu.SemaphoreType.DMA((n_w,)),
            pltpu.SemaphoreType.DMA((2, n_c)),
            pltpu.SemaphoreType.DMA((2, n_c)),
        ],
        compiler_params=pltpu.CompilerParams(vmem_limit_bytes=60 * 1024 * 1024),
        name='attend',
    )(positions, positions.reshape(1, rows), x, gamma.reshape(-1, LANES), beta.reshape(-1, LANES), w_rows, k_cache, v_cache)


def mlp_kernel(x_hbm, gamma_hbm, beta_hbm, ctx_hbm, wo_ref, wu_ref, wd_ref, out_ref,
               x_ref, gamma_ref, beta_ref, ctx_ref, small, wub, wcat, mlp_in, lhs, part, d2d_src, d2d_dst, cs32, csb, relay_a, relay_b, comb_a, comb_b,
               from_l, from_r, outb, usem, dsem, osem, send, recv, stored):
    n_u, _, cu = wub.shape
    n_b, _, cb = wcat.shape
    half, slab = d2d_src.shape[1], relay_a.shape[1]
    chips = half // slab
    rows = x_ref.shape[0]
    ctx_width = wo_ref.shape[0]
    groups = ctx_width // LANES
    me = lax.axis_index('tp')
    p, c = lax.div(me, 2), lax.rem(me, 2)
    right = 2 * lax.rem(p + 1, chips) + c
    left = 2 * lax.rem(p + chips - 1, chips) + c
    partner = me + 1 - 2 * c
    lo, hi = pl.ds(0, cb // 2), pl.ds(cb // 2, cb // 2)

    def up_copy(u):
        return pltpu.make_async_copy(wu_ref.at[:, pl.ds(u * cu, cu)], wub.at[u], usem.at[u])

    def down_copy(j):
        return pltpu.make_async_copy(wd_ref.at[:, pl.ds(j * cb, cb)], wcat.at[j, pl.ds(ctx_width, wd_ref.shape[0])], dsem.at[j])

    def out_copy(j):
        return pltpu.make_async_copy(wo_ref.at[:, pl.ds(j * cb, cb)], wcat.at[j, pl.ds(0, ctx_width)], osem.at[j])

    def fetch(n):
        if n < n_u:
            up_copy(n).start()
        elif n < n_u + n_b:
            out_copy(n - n_u).start()
            down_copy(n - n_u).start()

    first = [pltpu.make_async_copy(src, dst, small.at[n]) for n, (src, dst) in enumerate(
        ((x_hbm, x_ref), (gamma_hbm, gamma_ref), (beta_hbm, beta_ref), (ctx_hbm, ctx_ref)))]
    for copy in first:
        copy.start()
    for n in range(AHEAD):
        fetch(n)

    barrier = pltpu.get_barrier_semaphore()
    for peer in (right, left, partner):
        pl.semaphore_signal(barrier, inc=1, device_id={'tp': peer}, device_id_type=MESH)

    def in_half(q):
        return pl.ds(pl.multiple_of(lax.rem(p + q, chips) * slab, slab), slab)

    def in_rows(q, core):
        return pl.ds(pl.multiple_of(core * half + lax.rem(p + q, chips) * slab, slab), slab)

    def remote(kind, j):
        mine, before, after, far = (in_rows(q, c) for q in (0, chips - 1, 1, 2))
        src, dst, peer = (
            (d2d_src.at[j], d2d_dst.at[j], partner),
            (csb.at[j, in_half(2), lo], relay_a.at[j], right),
            (csb.at[j, in_half(2), hi], relay_b.at[j], left),
            (csb.at[j, in_half(1), hi], from_l.at[j, :, hi], right),
            (csb.at[j, in_half(chips - 1), lo], from_r.at[j, :, lo], left),
            (comb_a.at[j], from_l.at[j, :, lo], right),
            (comb_b.at[j], from_r.at[j, :, hi], left),
            (outb.at[j, mine], outb.at[j, mine], right),
            (outb.at[j, mine], outb.at[j, mine], left),
            (outb.at[j, mine], outb.at[j, mine], partner),
            (outb.at[j, before, lo], outb.at[j, before, lo], right),
            (outb.at[j, after, hi], outb.at[j, after, hi], left),
            (outb.at[j, before], outb.at[j, before], partner),
            (outb.at[j, after], outb.at[j, after], partner),
            (outb.at[j, far], outb.at[j, far], partner),
        )[kind]
        return pltpu.make_async_remote_copy(src_ref=src, dst_ref=dst, send_sem=send.at[kind, j], recv_sem=recv.at[kind, j],
                                            device_id={'tp': peer}, device_id_type=MESH)

    for copy in first:
        copy.wait()
    norm_into(x_ref, gamma_ref, beta_ref, mlp_in)
    for g in range(groups):
        lhs[:, g * LANES:(g + 1) * LANES] = ctx_ref[pl.ds(g, rows, stride=groups), :].astype(BF16)

    for u in range(n_u):
        up_copy(u).wait()
        fetch(u + AHEAD)
        z = jnp.dot(mlp_in[...], wub[u], preferred_element_type=F32)
        at = ctx_width + u * cu
        lhs[:, at:at + cu] = (0.5 * z * (1.0 + lax.erf(z * 0.5 ** 0.5))).astype(BF16)

    pl.semaphore_wait(barrier, 3)

    own_half = pl.ds(pl.multiple_of(c * half, half), half)
    other_half = pl.ds(pl.multiple_of((1 - c) * half, half), half)

    def compute(j):
        out_copy(j).wait()
        down_copy(j).wait()
        fetch(n_u + j + AHEAD)
        part[j] = jnp.dot(lhs[...], wcat[j], preferred_element_type=F32)
        d2d_src[j] = part[j, other_half].astype(BF16)
        remote(0, j).start()

    def chip_sum(j):
        remote(0, j).wait_recv()
        y = part[j, own_half] + d2d_dst[j].astype(F32)
        cs32[j] = y
        csb[j] = y.astype(BF16)
        for kind in (1, 2, 3, 4):
            remote(kind, j).start()

    def combine(j):
        remote(1, j).wait_recv()
        comb_a[j] = (cs32[j, in_half(1), lo] + relay_a[j].astype(F32)).astype(BF16)
        remote(5, j).start()
        remote(2, j).wait_recv()
        comb_b[j] = (cs32[j, in_half(chips - 1), hi] + relay_b[j].astype(F32)).astype(BF16)
        remote(6, j).start()

    def finish(j):
        for kind in (3, 4, 5, 6):
            remote(kind, j).wait_recv()
        mine = in_rows(0, c)
        y = cs32[j, in_half(0)] + from_l[j].astype(F32) + from_r[j].astype(F32)
        outb[j, mine] = (x_ref[mine, j * cb:(j + 1) * cb].astype(F32) + y).astype(BF16)
        for kind in (7, 8, 9):
            remote(kind, j).start()

    def forward(j):
        remote(7, j).wait_recv()
        remote(10, j).start()
        remote(12, j).start()
        remote(8, j).wait_recv()
        remote(11, j).start()
        remote(13, j).start()

    def share(j):
        remote(10, j).wait_recv()
        remote(11, j).wait_recv()
        remote(14, j).start()

    def store(j):
        return pltpu.make_async_copy(outb.at[j], out_ref.at[:, pl.ds(j * cb, cb)], stored.at[j])

    def collect(j):
        for kind in (9, 12, 13, 14):
            remote(kind, j).wait_recv()
        store(j).start()

    stages = ((compute, 0.0), (chip_sum, 1.4), (combine, 3.8), (finish, 6.2), (forward, 8.6), (share, 11.0), (collect, 12.4))
    plan = sorted((j * BLOCK_US + after, n, j) for n, (_, after) in enumerate(stages) for j in range(n_b))
    for _, n, j in plan:
        stages[n][0](j)
    for j in range(n_b):
        for kind in range(15):
            remote(kind, j).wait_send()
        store(j).wait()


def mlp_and_sum(mesh, x, gamma, beta, context, w_out, w_up, w_down):
    rows, width = x.shape
    hidden = w_up.shape[1]
    ctx_width = w_out.shape[0]
    chips = mesh.shape['tp'] // 2
    assert chips == 4
    n_u, n_b = hidden // UP_COLS, width // OUT_COLS
    half, slab = rows // 2, rows // 2 // chips

    def block(dtype, *shape):
        return pltpu.VMEM((n_b,) + shape, dtype)

    return pl.pallas_call(
        mlp_kernel,
        out_shape=jax.ShapeDtypeStruct(x.shape, x.dtype),
        in_specs=[HBM] * 7,
        out_specs=HBM,
        scratch_shapes=[
            pltpu.VMEM((rows, width), BF16),
            pltpu.VMEM((width // LANES, LANES), F32),
            pltpu.VMEM((width // LANES, LANES), F32),
            pltpu.VMEM(context.shape, F32),
            pltpu.SemaphoreType.DMA((4,)),
            pltpu.VMEM((n_u, width, UP_COLS), BF16),
            block(BF16, ctx_width + hidden, OUT_COLS),
            pltpu.VMEM((rows, width), BF16),
            pltpu.VMEM((rows, ctx_width + hidden), BF16),
            block(F32, rows, OUT_COLS),
            block(BF16, half, OUT_COLS),
            block(BF16, half, OUT_COLS),
            block(F32, half, OUT_COLS),
            block(BF16, half, OUT_COLS),
            block(BF16, slab, OUT_COLS // 2),
            block(BF16, slab, OUT_COLS // 2),
            block(BF16, slab, OUT_COLS // 2),
            block(BF16, slab, OUT_COLS // 2),
            block(BF16, slab, OUT_COLS),
            block(BF16, slab, OUT_COLS),
            block(BF16, rows, OUT_COLS),
            pltpu.SemaphoreType.DMA((n_u,)),
            pltpu.SemaphoreType.DMA((n_b,)),
            pltpu.SemaphoreType.DMA((n_b,)),
            pltpu.SemaphoreType.DMA((15, n_b)),
            pltpu.SemaphoreType.DMA((15, n_b)),
            pltpu.SemaphoreType.DMA((n_b,)),
        ],
        compiler_params=pltpu.CompilerParams(vmem_limit_bytes=60 * 1024 * 1024, collective_id=0, has_side_effects=True),
        name='mlp_and_sum',
    )(x, gamma.reshape(-1, LANES), beta.reshape(-1, LANES), context, w_out, w_up, w_down)


def solution(mesh):
    row_spec = P('dp', None)
    vec_spec = P(None)
    cache_spec = P('dp', 'tp', None, None)

    def device_step(x, ln_attn_gamma, ln_attn_beta, ln_mlp_gamma, ln_mlp_beta, w_qkv, w_out, w_up, w_down, k_cache, v_cache, positions):
        context, keys_all, values_all = attend(x, ln_attn_gamma, ln_attn_beta, w_qkv, k_cache, v_cache, positions)
        layer_out = mlp_and_sum(mesh, x, ln_mlp_gamma, ln_mlp_beta, context, w_out.reshape(-1, x.shape[1]), w_up, w_down)
        return layer_out, keys_all, values_all

    return jax.shard_map(device_step, mesh=mesh, in_specs=(row_spec, vec_spec, vec_spec, vec_spec, vec_spec, P(None, 'tp', None, None), P('tp', None, None, None), P(None, 'tp'), P('tp', None), cache_spec, cache_spec, P('dp')), out_specs=(row_spec, cache_spec, cache_spec), check_vma=False)
```

```python
import math

import jax
import jax.numpy as jnp
from jax import lax
from jax.experimental import pallas as pl
from jax.experimental.pallas import tpu as pltpu
from jax.sharding import PartitionSpec as P

LN_EPS = 1e-5
ROPE_BASE = 10000.0
NEG_BIG = -1e30
LANES = 128
ROWS_PER_CHUNK = 8
W_CHUNK = 256
W_AHEAD = 8
KV_AHEAD = 6
UP_COLS = 256
AHEAD = 2
OUT_COLS = 512
BLOCK_US = 0.9
F32 = jnp.float32
BF16 = jnp.bfloat16
HBM = pl.BlockSpec(memory_space=pltpu.HBM)
MESH = pl.DeviceIdType.MESH


def norm_into(x_ref, gamma_ref, beta_ref, dst_ref):
    rows, width = x_ref.shape
    tiles = width // LANES

    def tile(c):
        return x_ref[:, pl.ds(pl.multiple_of(c * LANES, LANES), LANES)].astype(F32)

    zero = jnp.zeros((rows, LANES), F32)
    total = lax.fori_loop(0, tiles, lambda c, s: s + tile(c), zero, unroll=4)
    mean = jnp.sum(total, axis=-1, keepdims=True) / width

    def square(c, s):
        d = tile(c) - mean
        return s + d * d

    var = jnp.sum(lax.fori_loop(0, tiles, square, zero, unroll=4), axis=-1, keepdims=True) / width
    inv = lax.rsqrt(var + LN_EPS)

    def write(c, carry):
        y = (tile(c) - mean) * inv * gamma_ref[pl.ds(c, 1), :] + beta_ref[pl.ds(c, 1), :]
        dst_ref[:, pl.ds(pl.multiple_of(c * LANES, LANES), LANES)] = y.astype(BF16)
        return carry

    lax.fori_loop(0, tiles, write, 0, unroll=4)


def attention_kernel(pos_hbm, pos_row_hbm, x_hbm, gamma_hbm, beta_hbm, w_ref, k_ref, v_ref, ctx_hbm, ko_ref, vo_ref,
                     pos_ref, pos_row, x_ref, gamma_ref, beta_ref, ctx_ref,
                     wbuf, wf, acc, attn, q_s, kn_s, vn_s, kbuf, vbuf, small, wsem, insem, outsem):
    rows, width = x_ref.shape
    _, groups, slots, head = k_ref.shape
    cols = 3 * groups
    n_w = width // W_CHUNK
    n_c = rows // ROWS_PER_CHUNK
    wrows = W_CHUNK * cols

    def w_copy(c):
        at = pl.ds(pl.multiple_of(c * wrows, wrows), wrows)
        return pltpu.make_async_copy(w_ref.at[at], wbuf.at[at], wsem.at[c])

    def io(i, which, out):
        hbm_in, hbm_out, buf = ((k_ref, ko_ref, kbuf), (v_ref, vo_ref, vbuf))[which]
        at = pl.ds(i * ROWS_PER_CHUNK, ROWS_PER_CHUNK)
        if out:
            return pltpu.make_async_copy(buf.at[at], hbm_out.at[at], outsem.at[which, i])
        return pltpu.make_async_copy(hbm_in.at[at], buf.at[at], insem.at[which, i])

    def kv_start(i):
        io(i, 0, False).start(priority=1)
        io(i, 1, False).start(priority=1)

    first = [pltpu.make_async_copy(src, dst, small.at[n]) for n, (src, dst) in enumerate(
        ((x_hbm, x_ref), (gamma_hbm, gamma_ref), (beta_hbm, beta_ref), (pos_row_hbm, pos_row), (pos_hbm, pos_ref)))]
    for copy in first:
        copy.start()
    for c in range(W_AHEAD):
        w_copy(c).start(priority=1)
    for copy in first:
        copy.wait()

    norm_into(x_ref, gamma_ref, beta_ref, attn)
    acc[...] = jnp.zeros_like(acc)

    def project(c, carry):
        w_copy(c).wait()

        @pl.when(c + W_AHEAD < n_w)
        def _():
            w_copy(c + W_AHEAD).start(priority=1)

        @pl.when(c >= n_w - KV_AHEAD)
        def _():
            kv_start(c - (n_w - KV_AHEAD))

        wf[...] = wbuf[pl.ds(pl.multiple_of(c * wrows, wrows), wrows), :].astype(F32)
        lhs = attn[:, pl.ds(pl.multiple_of(c * W_CHUNK, W_CHUNK), W_CHUNK)]
        for n in range(0, cols, 2):
            rhs = jnp.concatenate(
                [wf[pl.ds(n + e, W_CHUNK, stride=cols), :].astype(BF16) for e in range(2)], axis=1)
            acc[:, n * head:(n + 2) * head] += jnp.dot(lhs, rhs, preferred_element_type=F32)
        return carry

    lax.fori_loop(0, n_w, project, 0)

    lane = lax.broadcasted_iota(jnp.int32, (rows, head), 1)
    freq = jnp.exp(lax.rem(lane, head // 2).astype(F32) * (-2.0 * math.log(ROPE_BASE) / head))
    angle = jnp.broadcast_to(pos_row[...].astype(F32), (rows, rows)).T * freq
    cos_t = jnp.cos(angle)
    sin_t = jnp.where(lane < head // 2, -1.0, 1.0) * jnp.sin(angle)

    def rotate(u):
        u = u.astype(BF16).astype(F32)
        return (u * cos_t + pltpu.roll(u, head // 2, 1) * sin_t).astype(BF16).astype(F32)

    for g in range(groups):
        at = pl.ds(g, rows, stride=groups)
        q_s[at, :] = rotate(acc[:, g * head:(g + 1) * head])
        kn_s[at, :] = rotate(acc[:, (groups + g) * head:(groups + g + 1) * head])
        vn_s[at, :] = acc[:, (2 * groups + g) * head:(2 * groups + g + 1) * head].astype(BF16).astype(F32)

    row16 = lax.broadcasted_iota(jnp.int32, (16, head), 0)
    per_chunk = ROWS_PER_CHUNK * groups
    slot_id = lax.broadcasted_iota(jnp.int32, (slots, per_chunk), 0)
    lane_id = lax.broadcasted_iota(jnp.int32, (slots, per_chunk), 1)
    scale = head ** -0.5

    def chunk(i, carry):
        io(i, 0, False).wait()
        io(i, 1, False).wait()

        @pl.when(i + KV_AHEAD < n_c)
        def _():
            kv_start(i + KV_AHEAD)

        def write_row(r, carry):
            b = i * ROWS_PER_CHUNK + r
            pos = pos_ref[b]
            base = pl.multiple_of((pos // 16) * 16, 16)
            hit = row16 == pos - base
            for g in range(groups):
                for buf, new in ((kbuf, kn_s), (vbuf, vn_s)):
                    old = buf[b, g, pl.ds(base, 16), :].astype(F32)
                    row = new[pl.ds(b * groups + g, 1), :]
                    buf[b, g, pl.ds(base, 16), :] = jnp.where(hit, row, old).astype(BF16)
            return carry

        lax.fori_loop(0, ROWS_PER_CHUNK, write_row, 0, unroll=True)
        io(i, 0, True).start()
        io(i, 1, True).start()

        at = pl.ds(pl.multiple_of(i * per_chunk, per_chunk), per_chunk)
        queries = q_s[at, :].astype(BF16)
        s = jnp.zeros((slots, per_chunk), F32)
        limit = jnp.zeros((slots, per_chunk), jnp.int32)
        for r in range(ROWS_PER_CHUNK):
            b = i * ROWS_PER_CHUNK + r
            every = lax.dot_general(kbuf[b].reshape(groups * slots, head), queries, (((1,), (1,)), ((), ())),
                                    preferred_element_type=F32)
            for g in range(groups):
                s = jnp.where(lane_id == r * groups + g, every[g * slots:(g + 1) * slots], s)
            limit = jnp.where(lane_id >= r * groups, pos_ref[b], limit)
        s = jnp.where(slot_id <= limit, s * scale, NEG_BIG)
        e = jnp.exp(s - jnp.max(s, axis=0, keepdims=True))
        p = (e / jnp.sum(e, axis=0, keepdims=True)).astype(BF16).astype(F32)
        for r in range(ROWS_PER_CHUNK):
            b = i * ROWS_PER_CHUNK + r
            for g in range(groups):
                n = r * groups + g
                weighted = jnp.broadcast_to(p[:, n:n + 1], (slots, head)) * vbuf[b, g].astype(F32)
                ctx_ref[pl.ds(b * groups + g, 1), :] = jnp.sum(weighted, axis=0, keepdims=True).astype(BF16).astype(F32)
        return carry

    lax.fori_loop(0, n_c, chunk, 0)
    ctx_out = pltpu.make_async_copy(ctx_ref, ctx_hbm, small.at[0])
    ctx_out.start()
    for i in range(n_c):
        io(i, 0, True).wait()
        io(i, 1, True).wait()
    ctx_out.wait()


def attend(x, gamma, beta, w_qkv, k_cache, v_cache, positions):
    rows, width = x.shape
    _, groups, slots, head = k_cache.shape
    cols = 3 * groups
    w_rows = jnp.transpose(w_qkv, (0, 2, 1, 3)).reshape(width * cols, head)
    n_w, n_c = width // W_CHUNK, rows // ROWS_PER_CHUNK
    return pl.pallas_call(
        attention_kernel,
        out_shape=[jax.ShapeDtypeStruct((rows * groups, head), F32),
                   jax.ShapeDtypeStruct(k_cache.shape, k_cache.dtype),
                   jax.ShapeDtypeStruct(v_cache.shape, v_cache.dtype)],
        in_specs=[HBM] * 8,
        out_specs=[HBM] * 3,
        scratch_shapes=[
            pltpu.SMEM((rows,), jnp.int32),
            pltpu.VMEM((1, rows), jnp.int32),
            pltpu.VMEM((rows, width), BF16),
            pltpu.VMEM((width // LANES, LANES), F32),
            pltpu.VMEM((width // LANES, LANES), F32),
            pltpu.VMEM((rows * groups, head), F32),
            pltpu.VMEM((width * cols, head), BF16),
            pltpu.VMEM((W_CHUNK * cols, head), F32),
            pltpu.VMEM((rows, cols * head), F32),
            pltpu.VMEM((rows, width), BF16),
            pltpu.VMEM((rows * groups, head), F32),
            pltpu.VMEM((rows * groups, head), F32),
            pltpu.VMEM((rows * groups, head), F32),
            pltpu.VMEM(k_cache.shape, BF16),
            pltpu.VMEM(v_cache.shape, BF16),
            pltpu.SemaphoreType.DMA((5,)),
            pltpu.SemaphoreType.DMA((n_w,)),
            pltpu.SemaphoreType.DMA((2, n_c)),
            pltpu.SemaphoreType.DMA((2, n_c)),
        ],
        compiler_params=pltpu.CompilerParams(vmem_limit_bytes=60 * 1024 * 1024),
        name='attend',
    )(positions, positions.reshape(1, rows), x, gamma.reshape(-1, LANES), beta.reshape(-1, LANES), w_rows, k_cache, v_cache)


def mlp_kernel(x_hbm, gamma_hbm, beta_hbm, ctx_hbm, wo_ref, wu_ref, wd_ref, out_ref,
               x_ref, gamma_ref, beta_ref, ctx_ref, small, wub, wcat, mlp_in, lhs, part, d2d_src, d2d_dst, cs32, csb, relay_a, relay_b, comb_a, comb_b,
               from_l, from_r, outb, usem, dsem, osem, send, recv, stored):
    n_u, _, cu = wub.shape
    n_b, _, cb = wcat.shape
    half, slab = d2d_src.shape[1], relay_a.shape[1]
    chips = half // slab
    rows = x_ref.shape[0]
    ctx_width = wo_ref.shape[0]
    groups = ctx_width // LANES
    me = lax.axis_index('tp')
    p, c = lax.div(me, 2), lax.rem(me, 2)
    right = 2 * lax.rem(p + 1, chips) + c
    left = 2 * lax.rem(p + chips - 1, chips) + c
    partner = me + 1 - 2 * c
    lo, hi = pl.ds(0, cb // 2), pl.ds(cb // 2, cb // 2)

    def up_copy(u):
        return pltpu.make_async_copy(wu_ref.at[:, pl.ds(u * cu, cu)], wub.at[u], usem.at[u])

    def down_copy(j):
        return pltpu.make_async_copy(wd_ref.at[:, pl.ds(j * cb, cb)], wcat.at[j, pl.ds(ctx_width, wd_ref.shape[0])], dsem.at[j])

    def out_copy(j):
        return pltpu.make_async_copy(wo_ref.at[:, pl.ds(j * cb, cb)], wcat.at[j, pl.ds(0, ctx_width)], osem.at[j])

    def fetch(n):
        if n < n_u:
            up_copy(n).start()
        elif n < n_u + n_b:
            out_copy(n - n_u).start()
            down_copy(n - n_u).start()

    first = [pltpu.make_async_copy(src, dst, small.at[n]) for n, (src, dst) in enumerate(
        ((x_hbm, x_ref), (gamma_hbm, gamma_ref), (beta_hbm, beta_ref), (ctx_hbm, ctx_ref)))]
    for copy in first:
        copy.start()
    for n in range(AHEAD):
        fetch(n)

    barrier = pltpu.get_barrier_semaphore()
    for peer in (right, left, partner):
        pl.semaphore_signal(barrier, inc=1, device_id={'tp': peer}, device_id_type=MESH)

    def in_half(q):
        return pl.ds(pl.multiple_of(lax.rem(p + q, chips) * slab, slab), slab)

    def in_rows(q, core):
        return pl.ds(pl.multiple_of(core * half + lax.rem(p + q, chips) * slab, slab), slab)

    def remote(kind, j):
        mine, before, after, far = (in_rows(q, c) for q in (0, chips - 1, 1, 2))
        src, dst, peer = (
            (d2d_src.at[j], d2d_dst.at[j], partner),
            (csb.at[j, in_half(2), lo], relay_a.at[j], right),
            (csb.at[j, in_half(2), hi], relay_b.at[j], left),
            (csb.at[j, in_half(1), hi], from_l.at[j, :, hi], right),
            (csb.at[j, in_half(chips - 1), lo], from_r.at[j, :, lo], left),
            (comb_a.at[j], from_l.at[j, :, lo], right),
            (comb_b.at[j], from_r.at[j, :, hi], left),
            (outb.at[j, mine], outb.at[j, mine], right),
            (outb.at[j, mine], outb.at[j, mine], left),
            (outb.at[j, mine], outb.at[j, mine], partner),
            (outb.at[j, before, lo], outb.at[j, before, lo], right),
            (outb.at[j, after, hi], outb.at[j, after, hi], left),
            (outb.at[j, before], outb.at[j, before], partner),
            (outb.at[j, after], outb.at[j, after], partner),
            (outb.at[j, far], outb.at[j, far], partner),
        )[kind]
        return pltpu.make_async_remote_copy(src_ref=src, dst_ref=dst, send_sem=send.at[kind, j], recv_sem=recv.at[kind, j],
                                            device_id={'tp': peer}, device_id_type=MESH)

    for copy in first:
        copy.wait()
    norm_into(x_ref, gamma_ref, beta_ref, mlp_in)
    for g in range(groups):
        lhs[:, g * LANES:(g + 1) * LANES] = ctx_ref[pl.ds(g, rows, stride=groups), :].astype(BF16)

    for u in range(n_u):
        up_copy(u).wait()
        fetch(u + AHEAD)
        z = jnp.dot(mlp_in[...], wub[u], preferred_element_type=F32)
        at = ctx_width + u * cu
        lhs[:, at:at + cu] = (0.5 * z * (1.0 + lax.erf(z * 0.5 ** 0.5))).astype(BF16)

    pl.semaphore_wait(barrier, 3)

    own_half = pl.ds(pl.multiple_of(c * half, half), half)
    other_half = pl.ds(pl.multiple_of((1 - c) * half, half), half)

    def compute(j):
        out_copy(j).wait()
        down_copy(j).wait()
        fetch(n_u + j + AHEAD)
        part[j] = jnp.dot(lhs[...], wcat[j], preferred_element_type=F32)
        d2d_src[j] = part[j, other_half].astype(BF16)
        remote(0, j).start()

    def chip_sum(j):
        remote(0, j).wait_recv()
        y = part[j, own_half] + d2d_dst[j].astype(F32)
        cs32[j] = y
        csb[j] = y.astype(BF16)
        for kind in (1, 2, 3, 4):
            remote(kind, j).start()

    def combine(j):
        remote(1, j).wait_recv()
        comb_a[j] = (cs32[j, in_half(1), lo] + relay_a[j].astype(F32)).astype(BF16)
        remote(5, j).start()
        remote(2, j).wait_recv()
        comb_b[j] = (cs32[j, in_half(chips - 1), hi] + relay_b[j].astype(F32)).astype(BF16)
        remote(6, j).start()

    def finish(j):
        for kind in (3, 4, 5, 6):
            remote(kind, j).wait_recv()
        mine = in_rows(0, c)
        y = cs32[j, in_half(0)] + from_l[j].astype(F32) + from_r[j].astype(F32)
        outb[j, mine] = (x_ref[mine, j * cb:(j + 1) * cb].astype(F32) + y).astype(BF16)
        for kind in (7, 8, 9):
            remote(kind, j).start()

    def forward(j):
        remote(7, j).wait_recv()
        remote(10, j).start()
        remote(12, j).start()
        remote(8, j).wait_recv()
        remote(11, j).start()
        remote(13, j).start()

    def share(j):
        remote(10, j).wait_recv()
        remote(11, j).wait_recv()
        remote(14, j).start()

    def store(j):
        return pltpu.make_async_copy(outb.at[j], out_ref.at[:, pl.ds(j * cb, cb)], stored.at[j])

    def collect(j):
        for kind in (9, 12, 13, 14):
            remote(kind, j).wait_recv()
        store(j).start()

    stages = ((compute, 0.0), (chip_sum, 1.4), (combine, 3.8), (finish, 6.2), (forward, 8.6), (share, 11.0), (collect, 12.4))
    plan = sorted((j * BLOCK_US + after, n, j) for n, (_, after) in enumerate(stages) for j in range(n_b))
    for _, n, j in plan:
        stages[n][0](j)
    for j in range(n_b):
        for kind in range(15):
            remote(kind, j).wait_send()
        store(j).wait()


def mlp_and_sum(mesh, x, gamma, beta, context, w_out, w_up, w_down):
    rows, width = x.shape
    hidden = w_up.shape[1]
    ctx_width = w_out.shape[0]
    chips = mesh.shape['tp'] // 2
    assert chips == 4
    n_u, n_b = hidden // UP_COLS, width // OUT_COLS
    half, slab = rows // 2, rows // 2 // chips

    def block(dtype, *shape):
        return pltpu.VMEM((n_b,) + shape, dtype)

    return pl.pallas_call(
        mlp_kernel,
        out_shape=jax.ShapeDtypeStruct(x.shape, x.dtype),
        in_specs=[HBM] * 7,
        out_specs=HBM,
        scratch_shapes=[
            pltpu.VMEM((rows, width), BF16),
            pltpu.VMEM((width // LANES, LANES), F32),
            pltpu.VMEM((width // LANES, LANES), F32),
            pltpu.VMEM(context.shape, F32),
            pltpu.SemaphoreType.DMA((4,)),
            pltpu.VMEM((n_u, width, UP_COLS), BF16),
            block(BF16, ctx_width + hidden, OUT_COLS),
            pltpu.VMEM((rows, width), BF16),
            pltpu.VMEM((rows, ctx_width + hidden), BF16),
            block(F32, rows, OUT_COLS),
            block(BF16, half, OUT_COLS),
            block(BF16, half, OUT_COLS),
            block(F32, half, OUT_COLS),
            block(BF16, half, OUT_COLS),
            block(BF16, slab, OUT_COLS // 2),
            block(BF16, slab, OUT_COLS // 2),
            block(BF16, slab, OUT_COLS // 2),
            block(BF16, slab, OUT_COLS // 2),
            block(BF16, slab, OUT_COLS),
            block(BF16, slab, OUT_COLS),
            block(BF16, rows, OUT_COLS),
            pltpu.SemaphoreType.DMA((n_u,)),
            pltpu.SemaphoreType.DMA((n_b,)),
            pltpu.SemaphoreType.DMA((n_b,)),
            pltpu.SemaphoreType.DMA((15, n_b)),
            pltpu.SemaphoreType.DMA((15, n_b)),
            pltpu.SemaphoreType.DMA((n_b,)),
        ],
        compiler_params=pltpu.CompilerParams(vmem_limit_bytes=60 * 1024 * 1024, collective_id=0, has_side_effects=True),
        name='mlp_and_sum',
    )(x, gamma.reshape(-1, LANES), beta.reshape(-1, LANES), context, w_out, w_up, w_down)


def solution(mesh):
    row_spec = P('dp', None)
    vec_spec = P(None)
    cache_spec = P('dp', 'tp', None, None)

    def device_step(x, ln_attn_gamma, ln_attn_beta, ln_mlp_gamma, ln_mlp_beta, w_qkv, w_out, w_up, w_down, k_cache, v_cache, positions):
        context, keys_all, values_all = attend(x, ln_attn_gamma, ln_attn_beta, w_qkv, k_cache, v_cache, positions)
        layer_out = mlp_and_sum(mesh, x, ln_mlp_gamma, ln_mlp_beta, context, w_out.reshape(-1, x.shape[1]), w_up, w_down)
        return layer_out, keys_all, values_all

    return jax.shard_map(device_step, mesh=mesh, in_specs=(row_spec, vec_spec, vec_spec, vec_spec, vec_spec, P(None, 'tp', None, None), P('tp', None, None, None), P(None, 'tp'), P('tp', None), cache_spec, cache_spec, P('dp')), out_specs=(row_spec, cache_spec, cache_spec), check_vma=False)
```

```python
import math

import jax
import jax.numpy as jnp
from jax import lax
from jax.experimental import pallas as pl
from jax.experimental.pallas import tpu as pltpu
from jax.sharding import PartitionSpec as P

LN_EPS = 1e-5
ROPE_BASE = 10000.0
NEG_BIG = -1e30
LANES = 128
ROWS_PER_CHUNK = 8
W_CHUNK = 256
W_AHEAD = 8
KV_AHEAD = 6
UP_COLS = 256
AHEAD = 2
OUT_COLS = 512
BLOCK_US = 0.9
F32 = jnp.float32
BF16 = jnp.bfloat16
HBM = pl.BlockSpec(memory_space=pltpu.HBM)
MESH = pl.DeviceIdType.MESH


def norm_into(x_ref, gamma_ref, beta_ref, dst_ref):
    rows, width = x_ref.shape
    tiles = width // LANES

    def tile(c):
        return x_ref[:, pl.ds(pl.multiple_of(c * LANES, LANES), LANES)].astype(F32)

    zero = jnp.zeros((rows, LANES), F32)
    total = lax.fori_loop(0, tiles, lambda c, s: s + tile(c), zero, unroll=4)
    mean = jnp.sum(total, axis=-1, keepdims=True) / width

    def square(c, s):
        d = tile(c) - mean
        return s + d * d

    var = jnp.sum(lax.fori_loop(0, tiles, square, zero, unroll=4), axis=-1, keepdims=True) / width
    inv = lax.rsqrt(var + LN_EPS)

    def write(c, carry):
        y = (tile(c) - mean) * inv * gamma_ref[pl.ds(c, 1), :] + beta_ref[pl.ds(c, 1), :]
        dst_ref[:, pl.ds(pl.multiple_of(c * LANES, LANES), LANES)] = y.astype(BF16)
        return carry

    lax.fori_loop(0, tiles, write, 0, unroll=4)


def attention_kernel(pos_hbm, pos_row_hbm, x_hbm, gamma_hbm, beta_hbm, w_ref, k_ref, v_ref, ctx_hbm, ko_ref, vo_ref,
                     pos_ref, pos_row, x_ref, gamma_ref, beta_ref, ctx_ref,
                     wbuf, wf, acc, attn, q_s, kn_s, vn_s, kbuf, vbuf, small, wsem, insem, outsem):
    rows, width = x_ref.shape
    _, groups, slots, head = k_ref.shape
    cols = 3 * groups
    n_w = width // W_CHUNK
    n_c = rows // ROWS_PER_CHUNK
    wrows = W_CHUNK * cols

    def w_copy(c):
        at = pl.ds(pl.multiple_of(c * wrows, wrows), wrows)
        return pltpu.make_async_copy(w_ref.at[at], wbuf.at[at], wsem.at[c])

    def io(i, which, out):
        hbm_in, hbm_out, buf = ((k_ref, ko_ref, kbuf), (v_ref, vo_ref, vbuf))[which]
        at = pl.ds(i * ROWS_PER_CHUNK, ROWS_PER_CHUNK)
        if out:
            return pltpu.make_async_copy(buf.at[at], hbm_out.at[at], outsem.at[which, i])
        return pltpu.make_async_copy(hbm_in.at[at], buf.at[at], insem.at[which, i])

    def kv_start(i):
        io(i, 0, False).start(priority=1)
        io(i, 1, False).start(priority=1)

    first = [pltpu.make_async_copy(src, dst, small.at[n]) for n, (src, dst) in enumerate(
        ((x_hbm, x_ref), (gamma_hbm, gamma_ref), (beta_hbm, beta_ref), (pos_row_hbm, pos_row), (pos_hbm, pos_ref)))]
    for copy in first:
        copy.start()
    for c in range(W_AHEAD):
        w_copy(c).start(priority=1)
    for copy in first:
        copy.wait()

    norm_into(x_ref, gamma_ref, beta_ref, attn)
    acc[...] = jnp.zeros_like(acc)

    def project(c, carry):
        w_copy(c).wait()

        @pl.when(c + W_AHEAD < n_w)
        def _():
            w_copy(c + W_AHEAD).start(priority=1)

        @pl.when(c >= n_w - KV_AHEAD)
        def _():
            kv_start(c - (n_w - KV_AHEAD))

        wf[...] = wbuf[pl.ds(pl.multiple_of(c * wrows, wrows), wrows), :].astype(F32)
        lhs = attn[:, pl.ds(pl.multiple_of(c * W_CHUNK, W_CHUNK), W_CHUNK)]
        for n in range(0, cols, 2):
            rhs = jnp.concatenate(
                [wf[pl.ds(n + e, W_CHUNK, stride=cols), :].astype(BF16) for e in range(2)], axis=1)
            acc[:, n * head:(n + 2) * head] += jnp.dot(lhs, rhs, preferred_element_type=F32)
        return carry

    lax.fori_loop(0, n_w, project, 0)

    lane = lax.broadcasted_iota(jnp.int32, (rows, head), 1)
    freq = jnp.exp(lax.rem(lane, head // 2).astype(F32) * (-2.0 * math.log(ROPE_BASE) / head))
    angle = jnp.broadcast_to(pos_row[...].astype(F32), (rows, rows)).T * freq
    cos_t = jnp.cos(angle)
    sin_t = jnp.where(lane < head // 2, -1.0, 1.0) * jnp.sin(angle)

    def rotate(u):
        u = u.astype(BF16).astype(F32)
        return (u * cos_t + pltpu.roll(u, head // 2, 1) * sin_t).astype(BF16).astype(F32)

    for g in range(groups):
        at = pl.ds(g, rows, stride=groups)
        q_s[at, :] = rotate(acc[:, g * head:(g + 1) * head])
        kn_s[at, :] = rotate(acc[:, (groups + g) * head:(groups + g + 1) * head])
        vn_s[at, :] = acc[:, (2 * groups + g) * head:(2 * groups + g + 1) * head].astype(BF16).astype(F32)

    row16 = lax.broadcasted_iota(jnp.int32, (16, head), 0)
    per_chunk = ROWS_PER_CHUNK * groups
    slot_id = lax.broadcasted_iota(jnp.int32, (slots, per_chunk), 0)
    lane_id = lax.broadcasted_iota(jnp.int32, (slots, per_chunk), 1)
    scale = head ** -0.5

    def chunk(i, carry):
        io(i, 0, False).wait()
        io(i, 1, False).wait()

        @pl.when(i + KV_AHEAD < n_c)
        def _():
            kv_start(i + KV_AHEAD)

        def write_row(r, carry):
            b = i * ROWS_PER_CHUNK + r
            pos = pos_ref[b]
            base = pl.multiple_of((pos // 16) * 16, 16)
            hit = row16 == pos - base
            for g in range(groups):
                for buf, new in ((kbuf, kn_s), (vbuf, vn_s)):
                    old = buf[b, g, pl.ds(base, 16), :].astype(F32)
                    row = new[pl.ds(b * groups + g, 1), :]
                    buf[b, g, pl.ds(base, 16), :] = jnp.where(hit, row, old).astype(BF16)
            return carry

        lax.fori_loop(0, ROWS_PER_CHUNK, write_row, 0, unroll=True)
        io(i, 0, True).start()
        io(i, 1, True).start()

        at = pl.ds(pl.multiple_of(i * per_chunk, per_chunk), per_chunk)
        queries = q_s[at, :].astype(BF16)
        s = jnp.zeros((slots, per_chunk), F32)
        limit = jnp.zeros((slots, per_chunk), jnp.int32)
        for r in range(ROWS_PER_CHUNK):
            b = i * ROWS_PER_CHUNK + r
            every = lax.dot_general(kbuf[b].reshape(groups * slots, head), queries, (((1,), (1,)), ((), ())),
                                    preferred_element_type=F32)
            for g in range(groups):
                s = jnp.where(lane_id == r * groups + g, every[g * slots:(g + 1) * slots], s)
            limit = jnp.where(lane_id >= r * groups, pos_ref[b], limit)
        s = jnp.where(slot_id <= limit, s * scale, NEG_BIG)
        e = jnp.exp(s - jnp.max(s, axis=0, keepdims=True))
        p = (e / jnp.sum(e, axis=0, keepdims=True)).astype(BF16).astype(F32)
        for r in range(ROWS_PER_CHUNK):
            b = i * ROWS_PER_CHUNK + r
            for g in range(groups):
                n = r * groups + g
                weighted = jnp.broadcast_to(p[:, n:n + 1], (slots, head)) * vbuf[b, g].astype(F32)
                ctx_ref[pl.ds(b * groups + g, 1), :] = jnp.sum(weighted, axis=0, keepdims=True).astype(BF16).astype(F32)
        return carry

    lax.fori_loop(0, n_c, chunk, 0)
    ctx_out = pltpu.make_async_copy(ctx_ref, ctx_hbm, small.at[0])
    ctx_out.start()
    for i in range(n_c):
        io(i, 0, True).wait()
        io(i, 1, True).wait()
    ctx_out.wait()


def attend(x, gamma, beta, w_qkv, k_cache, v_cache, positions):
    rows, width = x.shape
    _, groups, slots, head = k_cache.shape
    cols = 3 * groups
    w_rows = jnp.transpose(w_qkv, (0, 2, 1, 3)).reshape(width * cols, head)
    n_w, n_c = width // W_CHUNK, rows // ROWS_PER_CHUNK
    return pl.pallas_call(
        attention_kernel,
        out_shape=[jax.ShapeDtypeStruct((rows * groups, head), F32),
                   jax.ShapeDtypeStruct(k_cache.shape, k_cache.dtype),
                   jax.ShapeDtypeStruct(v_cache.shape, v_cache.dtype)],
        in_specs=[HBM] * 8,
        out_specs=[HBM] * 3,
        scratch_shapes=[
            pltpu.SMEM((rows,), jnp.int32),
            pltpu.VMEM((1, rows), jnp.int32),
            pltpu.VMEM((rows, width), BF16),
            pltpu.VMEM((width // LANES, LANES), F32),
            pltpu.VMEM((width // LANES, LANES), F32),
            pltpu.VMEM((rows * groups, head), F32),
            pltpu.VMEM((width * cols, head), BF16),
            pltpu.VMEM((W_CHUNK * cols, head), F32),
            pltpu.VMEM((rows, cols * head), F32),
            pltpu.VMEM((rows, width), BF16),
            pltpu.VMEM((rows * groups, head), F32),
            pltpu.VMEM((rows * groups, head), F32),
            pltpu.VMEM((rows * groups, head), F32),
            pltpu.VMEM(k_cache.shape, BF16),
            pltpu.VMEM(v_cache.shape, BF16),
            pltpu.SemaphoreType.DMA((5,)),
            pltpu.SemaphoreType.DMA((n_w,)),
            pltpu.SemaphoreType.DMA((2, n_c)),
            pltpu.SemaphoreType.DMA((2, n_c)),
        ],
        compiler_params=pltpu.CompilerParams(vmem_limit_bytes=60 * 1024 * 1024),
        name='attend',
    )(positions, positions.reshape(1, rows), x, gamma.reshape(-1, LANES), beta.reshape(-1, LANES), w_rows, k_cache, v_cache)


def mlp_kernel(x_hbm, gamma_hbm, beta_hbm, ctx_hbm, wo_ref, wu_ref, wd_ref, out_ref,
               x_ref, gamma_ref, beta_ref, ctx_ref, small, wub, wcat, mlp_in, lhs, part, d2d_src, d2d_dst, cs32, csb, inbox, outb, usem, dsem, osem, send, recv, stored):
    n_u, _, cu = wub.shape
    n_b, _, cb = wcat.shape
    half, slab = d2d_src.shape[1], inbox.shape[2]
    chips = half // slab
    rows = x_ref.shape[0]
    ctx_width = wo_ref.shape[0]
    groups = ctx_width // LANES
    me = lax.axis_index('tp')
    p, c = lax.div(me, 2), lax.rem(me, 2)
    others = (2, 1, 3)
    partner = me + 1 - 2 * c

    def same_core(q):
        return 2 * lax.rem(p + q, chips) + c

    def up_copy(u):
        return pltpu.make_async_copy(wu_ref.at[:, pl.ds(u * cu, cu)], wub.at[u], usem.at[u])

    def down_copy(j):
        return pltpu.make_async_copy(wd_ref.at[:, pl.ds(j * cb, cb)], wcat.at[j, pl.ds(ctx_width, wd_ref.shape[0])], dsem.at[j])

    def out_copy(j):
        return pltpu.make_async_copy(wo_ref.at[:, pl.ds(j * cb, cb)], wcat.at[j, pl.ds(0, ctx_width)], osem.at[j])

    def fetch(n):
        if n < n_u:
            up_copy(n).start()
        elif n < n_u + n_b:
            out_copy(n - n_u).start()
            down_copy(n - n_u).start()

    first = [pltpu.make_async_copy(src, dst, small.at[n]) for n, (src, dst) in enumerate(
        ((x_hbm, x_ref), (gamma_hbm, gamma_ref), (beta_hbm, beta_ref), (ctx_hbm, ctx_ref)))]
    for copy in first:
        copy.start()
    for n in range(AHEAD):
        fetch(n)

    barrier = pltpu.get_barrier_semaphore()
    for peer in tuple(same_core(q) for q in others) + (partner,):
        pl.semaphore_signal(barrier, inc=1, device_id={'tp': peer}, device_id_type=MESH)

    def in_half(q):
        return pl.ds(pl.multiple_of(lax.rem(p + q, chips) * slab, slab), slab)

    def in_rows(q, core):
        return pl.ds(pl.multiple_of(core * half + lax.rem(p + q, chips) * slab, slab), slab)

    def remote(kind, j):
        mine = in_rows(0, c)
        if kind == 0:
            src, dst, peer = d2d_src.at[j], d2d_dst.at[j], partner
        elif kind < 4:
            q = others[kind - 1]
            src, dst, peer = csb.at[j, in_half(q)], inbox.at[j, kind - 1], same_core(q)
        elif kind < 7:
            src, dst, peer = outb.at[j, mine], outb.at[j, mine], same_core(others[kind - 4])
        elif kind == 7:
            src, dst, peer = outb.at[j, mine], outb.at[j, mine], partner
        else:
            far = in_rows(chips - others[kind - 8], c)
            src, dst, peer = outb.at[j, far], outb.at[j, far], partner
        return pltpu.make_async_remote_copy(src_ref=src, dst_ref=dst, send_sem=send.at[kind, j], recv_sem=recv.at[kind, j],
                                            device_id={'tp': peer}, device_id_type=MESH)

    for copy in first:
        copy.wait()
    norm_into(x_ref, gamma_ref, beta_ref, mlp_in)
    for g in range(groups):
        lhs[:, g * LANES:(g + 1) * LANES] = ctx_ref[pl.ds(g, rows, stride=groups), :].astype(BF16)

    for u in range(n_u):
        up_copy(u).wait()
        fetch(u + AHEAD)
        z = jnp.dot(mlp_in[...], wub[u], preferred_element_type=F32)
        at = ctx_width + u * cu
        lhs[:, at:at + cu] = (0.5 * z * (1.0 + lax.erf(z * 0.5 ** 0.5))).astype(BF16)

    pl.semaphore_wait(barrier, 4)

    own_half = pl.ds(pl.multiple_of(c * half, half), half)
    other_half = pl.ds(pl.multiple_of((1 - c) * half, half), half)

    def compute(j):
        out_copy(j).wait()
        down_copy(j).wait()
        fetch(n_u + j + AHEAD)
        part[j] = jnp.dot(lhs[...], wcat[j], preferred_element_type=F32)
        d2d_src[j] = part[j, other_half].astype(BF16)
        remote(0, j).start()

    def chip_sum(j):
        remote(0, j).wait_recv()
        y = part[j, own_half] + d2d_dst[j].astype(F32)
        cs32[j] = y
        csb[j] = y.astype(BF16)
        for kind in (1, 2, 3):
            remote(kind, j).start()

    def finish(j):
        y = cs32[j, in_half(0)]
        for kind in (1, 2, 3):
            remote(kind, j).wait_recv()
            y += inbox[j, kind - 1].astype(F32)
        mine = in_rows(0, c)
        outb[j, mine] = (x_ref[mine, j * cb:(j + 1) * cb].astype(F32) + y).astype(BF16)
        for kind in (4, 5, 6, 7):
            remote(kind, j).start()

    def share(j):
        for kind in (4, 5, 6):
            remote(kind, j).wait_recv()
            remote(kind + 4, j).start()

    def store(j):
        return pltpu.make_async_copy(outb.at[j], out_ref.at[:, pl.ds(j * cb, cb)], stored.at[j])

    def collect(j):
        for kind in (7, 8, 9, 10):
            remote(kind, j).wait_recv()
        store(j).start()

    stages = ((compute, 0.0), (chip_sum, 1.4), (finish, 5.0), (share, 8.6), (collect, 10.0))
    plan = sorted((j * BLOCK_US + after, n, j) for n, (_, after) in enumerate(stages) for j in range(n_b))
    for _, n, j in plan:
        stages[n][0](j)
    for j in range(n_b):
        for kind in range(11):
            remote(kind, j).wait_send()
        store(j).wait()


def mlp_and_sum(mesh, x, gamma, beta, context, w_out, w_up, w_down):
    rows, width = x.shape
    hidden = w_up.shape[1]
    ctx_width = w_out.shape[0]
    chips = mesh.shape['tp'] // 2
    assert chips == 4
    n_u, n_b = hidden // UP_COLS, width // OUT_COLS
    half, slab = rows // 2, rows // 2 // chips

    def block(dtype, *shape):
        return pltpu.VMEM((n_b,) + shape, dtype)

    return pl.pallas_call(
        mlp_kernel,
        out_shape=jax.ShapeDtypeStruct(x.shape, x.dtype),
        in_specs=[HBM] * 7,
        out_specs=HBM,
        scratch_shapes=[
            pltpu.VMEM((rows, width), BF16),
            pltpu.VMEM((width // LANES, LANES), F32),
            pltpu.VMEM((width // LANES, LANES), F32),
            pltpu.VMEM(context.shape, F32),
            pltpu.SemaphoreType.DMA((4,)),
            pltpu.VMEM((n_u, width, UP_COLS), BF16),
            block(BF16, ctx_width + hidden, OUT_COLS),
            pltpu.VMEM((rows, width), BF16),
            pltpu.VMEM((rows, ctx_width + hidden), BF16),
            block(F32, rows, OUT_COLS),
            block(BF16, half, OUT_COLS),
            block(BF16, half, OUT_COLS),
            block(F32, half, OUT_COLS),
            block(BF16, half, OUT_COLS),
            block(BF16, chips - 1, slab, OUT_COLS),
            block(BF16, rows, OUT_COLS),
            pltpu.SemaphoreType.DMA((n_u,)),
            pltpu.SemaphoreType.DMA((n_b,)),
            pltpu.SemaphoreType.DMA((n_b,)),
            pltpu.SemaphoreType.DMA((11, n_b)),
            pltpu.SemaphoreType.DMA((11, n_b)),
            pltpu.SemaphoreType.DMA((n_b,)),
        ],
        compiler_params=pltpu.CompilerParams(vmem_limit_bytes=60 * 1024 * 1024, collective_id=0, has_side_effects=True),
        name='mlp_and_sum',
    )(x, gamma.reshape(-1, LANES), beta.reshape(-1, LANES), context, w_out, w_up, w_down)


def solution(mesh):
    row_spec = P('dp', None)
    vec_spec = P(None)
    cache_spec = P('dp', 'tp', None, None)

    def device_step(x, ln_attn_gamma, ln_attn_beta, ln_mlp_gamma, ln_mlp_beta, w_qkv, w_out, w_up, w_down, k_cache, v_cache, positions):
        context, keys_all, values_all = attend(x, ln_attn_gamma, ln_attn_beta, w_qkv, k_cache, v_cache, positions)
        layer_out = mlp_and_sum(mesh, x, ln_mlp_gamma, ln_mlp_beta, context, w_out.reshape(-1, x.shape[1]), w_up, w_down)
        return layer_out, keys_all, values_all

    return jax.shard_map(device_step, mesh=mesh, in_specs=(row_spec, vec_spec, vec_spec, vec_spec, vec_spec, P(None, 'tp', None, None), P('tp', None, None, None), P(None, 'tp'), P('tp', None), cache_spec, cache_spec, P('dp')), out_specs=(row_spec, cache_spec, cache_spec), check_vma=False)
```

```python
import math

import jax
import jax.numpy as jnp
from jax import lax
from jax.experimental import pallas as pl
from jax.experimental.pallas import tpu as pltpu
from jax.sharding import PartitionSpec as P

LN_EPS = 1e-5
ROPE_BASE = 10000.0
NEG_BIG = -1e30
LANES = 128
ROWS_PER_CHUNK = 8
W_CHUNK = 256
W_AHEAD = 16
KV_AHEAD = 12
UP_COLS = 256
AHEAD = 2
OUT_COLS = 512
BLOCK_US = 0.9
F32 = jnp.float32
BF16 = jnp.bfloat16
HBM = pl.BlockSpec(memory_space=pltpu.HBM)
MESH = pl.DeviceIdType.MESH


def norm_into(x_ref, gamma_ref, beta_ref, dst_ref):
    rows, width = x_ref.shape
    tiles = width // LANES

    def tile(c):
        return x_ref[:, pl.ds(pl.multiple_of(c * LANES, LANES), LANES)].astype(F32)

    zero = jnp.zeros((rows, LANES), F32)
    total = lax.fori_loop(0, tiles, lambda c, s: s + tile(c), zero, unroll=4)
    mean = jnp.sum(total, axis=-1, keepdims=True) / width

    def square(c, s):
        d = tile(c) - mean
        return s + d * d

    var = jnp.sum(lax.fori_loop(0, tiles, square, zero, unroll=4), axis=-1, keepdims=True) / width
    inv = lax.rsqrt(var + LN_EPS)

    def write(c, carry):
        y = (tile(c) - mean) * inv * gamma_ref[pl.ds(c, 1), :] + beta_ref[pl.ds(c, 1), :]
        dst_ref[:, pl.ds(pl.multiple_of(c * LANES, LANES), LANES)] = y.astype(BF16)
        return carry

    lax.fori_loop(0, tiles, write, 0, unroll=4)


def attention_kernel(pos_hbm, pos_row_hbm, x_hbm, gamma_hbm, beta_hbm, w_ref, k_ref, v_ref, ctx_hbm, ko_ref, vo_ref,
                     pos_ref, pos_row, x_ref, gamma_ref, beta_ref, ctx_ref,
                     wbuf, wf, acc, attn, q_s, kn_s, vn_s, kbuf, vbuf, small, wsem, insem, outsem):
    rows, width = x_ref.shape
    _, groups, slots, head = k_ref.shape
    cols = 3 * groups
    n_w = width // W_CHUNK
    n_c = rows // ROWS_PER_CHUNK
    wrows = W_CHUNK * cols

    def w_copy(c):
        at = pl.ds(pl.multiple_of(c * wrows, wrows), wrows)
        return pltpu.make_async_copy(w_ref.at[at], wbuf.at[at], wsem.at[c])

    def io(i, which, out):
        hbm_in, hbm_out, buf = ((k_ref, ko_ref, kbuf), (v_ref, vo_ref, vbuf))[which]
        at = pl.ds(i * ROWS_PER_CHUNK, ROWS_PER_CHUNK)
        if out:
            return pltpu.make_async_copy(buf.at[at], hbm_out.at[at], outsem.at[which, i])
        return pltpu.make_async_copy(hbm_in.at[at], buf.at[at], insem.at[which, i])

    def kv_start(i):
        io(i, 0, False).start(priority=1)
        io(i, 1, False).start(priority=1)

    first = [pltpu.make_async_copy(src, dst, small.at[n]) for n, (src, dst) in enumerate(
        ((x_hbm, x_ref), (gamma_hbm, gamma_ref), (beta_hbm, beta_ref), (pos_row_hbm, pos_row), (pos_hbm, pos_ref)))]
    for copy in first:
        copy.start()
    for c in range(W_AHEAD):
        w_copy(c).start(priority=1)
    for copy in first:
        copy.wait()

    norm_into(x_ref, gamma_ref, beta_ref, attn)
    acc[...] = jnp.zeros_like(acc)

    def project(c, carry):
        w_copy(c).wait()

        @pl.when(c + W_AHEAD < n_w)
        def _():
            w_copy(c + W_AHEAD).start(priority=1)

        @pl.when(c >= n_w - KV_AHEAD)
        def _():
            kv_start(c - (n_w - KV_AHEAD))

        wf[...] = wbuf[pl.ds(pl.multiple_of(c * wrows, wrows), wrows), :].astype(F32)
        lhs = attn[:, pl.ds(pl.multiple_of(c * W_CHUNK, W_CHUNK), W_CHUNK)]
        for n in range(0, cols, 2):
            rhs = jnp.concatenate(
                [wf[pl.ds(n + e, W_CHUNK, stride=cols), :].astype(BF16) for e in range(2)], axis=1)
            acc[:, n * head:(n + 2) * head] += jnp.dot(lhs, rhs, preferred_element_type=F32)
        return carry

    lax.fori_loop(0, n_w, project, 0)

    lane = lax.broadcasted_iota(jnp.int32, (rows, head), 1)
    freq = jnp.exp(lax.rem(lane, head // 2).astype(F32) * (-2.0 * math.log(ROPE_BASE) / head))
    angle = jnp.broadcast_to(pos_row[...].astype(F32), (rows, rows)).T * freq
    cos_t = jnp.cos(angle)
    sin_t = jnp.where(lane < head // 2, -1.0, 1.0) * jnp.sin(angle)

    def rotate(u):
        u = u.astype(BF16).astype(F32)
        return (u * cos_t + pltpu.roll(u, head // 2, 1) * sin_t).astype(BF16).astype(F32)

    for g in range(groups):
        at = pl.ds(g, rows, stride=groups)
        q_s[at, :] = rotate(acc[:, g * head:(g + 1) * head])
        kn_s[at, :] = rotate(acc[:, (groups + g) * head:(groups + g + 1) * head])
        vn_s[at, :] = acc[:, (2 * groups + g) * head:(2 * groups + g + 1) * head].astype(BF16).astype(F32)

    row16 = lax.broadcasted_iota(jnp.int32, (16, head), 0)
    per_chunk = ROWS_PER_CHUNK * groups
    slot_id = lax.broadcasted_iota(jnp.int32, (slots, per_chunk), 0)
    lane_id = lax.broadcasted_iota(jnp.int32, (slots, per_chunk), 1)
    scale = head ** -0.5

    def chunk(i, carry):
        io(i, 0, False).wait()
        io(i, 1, False).wait()

        @pl.when(i + KV_AHEAD < n_c)
        def _():
            kv_start(i + KV_AHEAD)

        def write_row(r, carry):
            b = i * ROWS_PER_CHUNK + r
            pos = pos_ref[b]
            base = pl.multiple_of((pos // 16) * 16, 16)
            hit = row16 == pos - base
            for g in range(groups):
                for buf, new in ((kbuf, kn_s), (vbuf, vn_s)):
                    old = buf[b, g, pl.ds(base, 16), :].astype(F32)
                    row = new[pl.ds(b * groups + g, 1), :]
                    buf[b, g, pl.ds(base, 16), :] = jnp.where(hit, row, old).astype(BF16)
            return carry

        lax.fori_loop(0, ROWS_PER_CHUNK, write_row, 0, unroll=True)
        io(i, 0, True).start()
        io(i, 1, True).start()

        at = pl.ds(pl.multiple_of(i * per_chunk, per_chunk), per_chunk)
        queries = q_s[at, :].astype(BF16)
        s = jnp.zeros((slots, per_chunk), F32)
        limit = jnp.zeros((slots, per_chunk), jnp.int32)
        for r in range(ROWS_PER_CHUNK):
            b = i * ROWS_PER_CHUNK + r
            every = lax.dot_general(kbuf[b].reshape(groups * slots, head), queries, (((1,), (1,)), ((), ())),
                                    preferred_element_type=F32)
            for g in range(groups):
                s = jnp.where(lane_id == r * groups + g, every[g * slots:(g + 1) * slots], s)
            limit = jnp.where(lane_id >= r * groups, pos_ref[b], limit)
        s = jnp.where(slot_id <= limit, s * scale, NEG_BIG)
        e = jnp.exp(s - jnp.max(s, axis=0, keepdims=True))
        p = (e / jnp.sum(e, axis=0, keepdims=True)).astype(BF16).astype(F32)
        for r in range(ROWS_PER_CHUNK):
            b = i * ROWS_PER_CHUNK + r
            for g in range(groups):
                n = r * groups + g
                weighted = jnp.broadcast_to(p[:, n:n + 1], (slots, head)) * vbuf[b, g].astype(F32)
                ctx_ref[pl.ds(b * groups + g, 1), :] = jnp.sum(weighted, axis=0, keepdims=True).astype(BF16).astype(F32)
        return carry

    lax.fori_loop(0, n_c, chunk, 0)
    ctx_out = pltpu.make_async_copy(ctx_ref, ctx_hbm, small.at[0])
    ctx_out.start()
    for i in range(n_c):
        io(i, 0, True).wait()
        io(i, 1, True).wait()
    ctx_out.wait()


def attend(x, gamma, beta, w_qkv, k_cache, v_cache, positions):
    rows, width = x.shape
    _, groups, slots, head = k_cache.shape
    cols = 3 * groups
    w_rows = jnp.transpose(w_qkv, (0, 2, 1, 3)).reshape(width * cols, head)
    n_w, n_c = width // W_CHUNK, rows // ROWS_PER_CHUNK
    return pl.pallas_call(
        attention_kernel,
        out_shape=[jax.ShapeDtypeStruct((rows * groups, head), F32),
                   jax.ShapeDtypeStruct(k_cache.shape, k_cache.dtype),
                   jax.ShapeDtypeStruct(v_cache.shape, v_cache.dtype)],
        in_specs=[HBM] * 8,
        out_specs=[HBM] * 3,
        scratch_shapes=[
            pltpu.SMEM((rows,), jnp.int32),
            pltpu.VMEM((1, rows), jnp.int32),
            pltpu.VMEM((rows, width), BF16),
            pltpu.VMEM((width // LANES, LANES), F32),
            pltpu.VMEM((width // LANES, LANES), F32),
            pltpu.VMEM((rows * groups, head), F32),
            pltpu.VMEM((width * cols, head), BF16),
            pltpu.VMEM((W_CHUNK * cols, head), F32),
            pltpu.VMEM((rows, cols * head), F32),
            pltpu.VMEM((rows, width), BF16),
            pltpu.VMEM((rows * groups, head), F32),
            pltpu.VMEM((rows * groups, head), F32),
            pltpu.VMEM((rows * groups, head), F32),
            pltpu.VMEM(k_cache.shape, BF16),
            pltpu.VMEM(v_cache.shape, BF16),
            pltpu.SemaphoreType.DMA((5,)),
            pltpu.SemaphoreType.DMA((n_w,)),
            pltpu.SemaphoreType.DMA((2, n_c)),
            pltpu.SemaphoreType.DMA((2, n_c)),
        ],
        compiler_params=pltpu.CompilerParams(vmem_limit_bytes=60 * 1024 * 1024),
        name='attend',
    )(positions, positions.reshape(1, rows), x, gamma.reshape(-1, LANES), beta.reshape(-1, LANES), w_rows, k_cache, v_cache)


def mlp_kernel(x_hbm, gamma_hbm, beta_hbm, ctx_hbm, wo_ref, wu_ref, wd_ref, out_ref,
               x_ref, gamma_ref, beta_ref, ctx_ref, small, wub, wcat, mlp_in, lhs, part, d2d_src, d2d_dst, cs32, csb, inbox, outb, usem, dsem, osem, send, recv):
    n_u, _, cu = wub.shape
    n_b, _, cb = wcat.shape
    half, slab = d2d_src.shape[1], inbox.shape[2]
    chips = half // slab
    rows = x_ref.shape[0]
    ctx_width = wo_ref.shape[0]
    groups = ctx_width // LANES
    me = lax.axis_index('tp')
    p, c = lax.div(me, 2), lax.rem(me, 2)
    others = (2, 1, 3)
    partner = me + 1 - 2 * c

    def same_core(q):
        return 2 * lax.rem(p + q, chips) + c

    def up_copy(u):
        return pltpu.make_async_copy(wu_ref.at[:, pl.ds(u * cu, cu)], wub.at[u], usem.at[u])

    def down_copy(j):
        return pltpu.make_async_copy(wd_ref.at[:, pl.ds(j * cb, cb)], wcat.at[j, pl.ds(ctx_width, wd_ref.shape[0])], dsem.at[j])

    def out_copy(j):
        return pltpu.make_async_copy(wo_ref.at[:, pl.ds(j * cb, cb)], wcat.at[j, pl.ds(0, ctx_width)], osem.at[j])

    def fetch(n):
        if n < n_u:
            up_copy(n).start()
        elif n < n_u + n_b:
            out_copy(n - n_u).start()
            down_copy(n - n_u).start()

    first = [pltpu.make_async_copy(src, dst, small.at[n]) for n, (src, dst) in enumerate(
        ((x_hbm, x_ref), (gamma_hbm, gamma_ref), (beta_hbm, beta_ref), (ctx_hbm, ctx_ref)))]
    for copy in first:
        copy.start()
    for n in range(AHEAD):
        fetch(n)

    barrier = pltpu.get_barrier_semaphore()
    for peer in tuple(same_core(q) for q in others) + (partner,):
        pl.semaphore_signal(barrier, inc=1, device_id={'tp': peer}, device_id_type=MESH)

    def in_half(q):
        return pl.ds(pl.multiple_of(lax.rem(p + q, chips) * slab, slab), slab)

    def in_rows(q, core):
        return pl.ds(pl.multiple_of(core * half + lax.rem(p + q, chips) * slab, slab), slab)

    def remote(kind, j):
        mine = in_rows(0, c)
        if kind == 0:
            src, dst, peer = d2d_src.at[j], d2d_dst.at[j], partner
        elif kind < 4:
            q = others[kind - 1]
            src, dst, peer = csb.at[j, in_half(q)], inbox.at[j, kind - 1], same_core(q)
        elif kind < 7:
            src, dst, peer = outb.at[j, mine], outb.at[j, mine], same_core(others[kind - 4])
        elif kind == 7:
            src, dst, peer = outb.at[j, mine], outb.at[j, mine], partner
        else:
            far = in_rows(chips - others[kind - 8], c)
            src, dst, peer = outb.at[j, far], outb.at[j, far], partner
        return pltpu.make_async_remote_copy(src_ref=src, dst_ref=dst, send_sem=send.at[kind, j], recv_sem=recv.at[kind, j],
                                            device_id={'tp': peer}, device_id_type=MESH)

    for copy in first:
        copy.wait()
    norm_into(x_ref, gamma_ref, beta_ref, mlp_in)
    for g in range(groups):
        lhs[:, g * LANES:(g + 1) * LANES] = ctx_ref[pl.ds(g, rows, stride=groups), :].astype(BF16)

    for u in range(n_u):
        up_copy(u).wait()
        fetch(u + AHEAD)
        z = jnp.dot(mlp_in[...], wub[u], preferred_element_type=F32)
        at = ctx_width + u * cu
        lhs[:, at:at + cu] = (0.5 * z * (1.0 + lax.erf(z * 0.5 ** 0.5))).astype(BF16)

    pl.semaphore_wait(barrier, 4)

    own_half = pl.ds(pl.multiple_of(c * half, half), half)
    other_half = pl.ds(pl.multiple_of((1 - c) * half, half), half)

    def compute(j):
        out_copy(j).wait()
        down_copy(j).wait()
        fetch(n_u + j + AHEAD)
        part[j] = jnp.dot(lhs[...], wcat[j], preferred_element_type=F32)
        d2d_src[j] = part[j, other_half].astype(BF16)
        remote(0, j).start()

    def chip_sum(j):
        remote(0, j).wait_recv()
        y = part[j, own_half] + d2d_dst[j].astype(F32)
        cs32[j] = y
        csb[j] = y.astype(BF16)
        for kind in (1, 2, 3):
            remote(kind, j).start()

    def finish(j):
        y = cs32[j, in_half(0)]
        for kind in (1, 2, 3):
            remote(kind, j).wait_recv()
            y += inbox[j, kind - 1].astype(F32)
        mine = in_rows(0, c)
        outb[j, mine] = (x_ref[mine, j * cb:(j + 1) * cb].astype(F32) + y).astype(BF16)
        for kind in (4, 5, 6, 7):
            remote(kind, j).start()

    def share(j):
        for kind in (4, 5, 6):
            remote(kind, j).wait_recv()
            remote(kind + 4, j).start()

    def collect(j):
        for kind in (7, 8, 9, 10):
            remote(kind, j).wait_recv()
        out_ref[:, j * cb:(j + 1) * cb] = outb[j]

    stages = ((compute, 0.0), (chip_sum, 1.4), (finish, 5.0), (share, 8.6), (collect, 10.0))
    plan = sorted((j * BLOCK_US + after, n, j) for n, (_, after) in enumerate(stages) for j in range(n_b))
    for _, n, j in plan:
        stages[n][0](j)
    for j in range(n_b):
        for kind in range(11):
            remote(kind, j).wait_send()


def mlp_and_sum(mesh, x, gamma, beta, context, w_out, w_up, w_down):
    rows, width = x.shape
    hidden = w_up.shape[1]
    ctx_width = w_out.shape[0]
    chips = mesh.shape['tp'] // 2
    assert chips == 4
    n_u, n_b = hidden // UP_COLS, width // OUT_COLS
    half, slab = rows // 2, rows // 2 // chips

    def block(dtype, *shape):
        return pltpu.VMEM((n_b,) + shape, dtype)

    return pl.pallas_call(
        mlp_kernel,
        out_shape=jax.ShapeDtypeStruct(x.shape, x.dtype),
        in_specs=[HBM] * 7,
        out_specs=pl.BlockSpec(memory_space=pltpu.VMEM),
        scratch_shapes=[
            pltpu.VMEM((rows, width), BF16),
            pltpu.VMEM((width // LANES, LANES), F32),
            pltpu.VMEM((width // LANES, LANES), F32),
            pltpu.VMEM(context.shape, F32),
            pltpu.SemaphoreType.DMA((4,)),
            pltpu.VMEM((n_u, width, UP_COLS), BF16),
            block(BF16, ctx_width + hidden, OUT_COLS),
            pltpu.VMEM((rows, width), BF16),
            pltpu.VMEM((rows, ctx_width + hidden), BF16),
            block(F32, rows, OUT_COLS),
            block(BF16, half, OUT_COLS),
            block(BF16, half, OUT_COLS),
            block(F32, half, OUT_COLS),
            block(BF16, half, OUT_COLS),
            block(BF16, chips - 1, slab, OUT_COLS),
            block(BF16, rows, OUT_COLS),
            pltpu.SemaphoreType.DMA((n_u,)),
            pltpu.SemaphoreType.DMA((n_b,)),
            pltpu.SemaphoreType.DMA((n_b,)),
            pltpu.SemaphoreType.DMA((11, n_b)),
            pltpu.SemaphoreType.DMA((11, n_b)),
        ],
        compiler_params=pltpu.CompilerParams(vmem_limit_bytes=48 * 1024 * 1024, collective_id=0, has_side_effects=True),
        name='mlp_and_sum',
    )(x, gamma.reshape(-1, LANES), beta.reshape(-1, LANES), context, w_out, w_up, w_down)


def solution(mesh):
    row_spec = P('dp', None)
    vec_spec = P(None)
    cache_spec = P('dp', 'tp', None, None)

    def device_step(x, ln_attn_gamma, ln_attn_beta, ln_mlp_gamma, ln_mlp_beta, w_qkv, w_out, w_up, w_down, k_cache, v_cache, positions):
        context, keys_all, values_all = attend(x, ln_attn_gamma, ln_attn_beta, w_qkv, k_cache, v_cache, positions)
        layer_out = mlp_and_sum(mesh, x, ln_mlp_gamma, ln_mlp_beta, context, w_out.reshape(-1, x.shape[1]), w_up, w_down)
        return layer_out, keys_all, values_all

    return jax.shard_map(device_step, mesh=mesh, in_specs=(row_spec, vec_spec, vec_spec, vec_spec, vec_spec, P(None, 'tp', None, None), P('tp', None, None, None), P(None, 'tp'), P('tp', None), cache_spec, cache_spec, P('dp')), out_specs=(row_spec, cache_spec, cache_spec), check_vma=False)
```

```python
import math

import jax
import jax.numpy as jnp
from jax import lax
from jax.experimental import pallas as pl
from jax.experimental.pallas import tpu as pltpu
from jax.sharding import PartitionSpec as P

LN_EPS = 1e-5
ROPE_BASE = 10000.0
NEG_BIG = -1e30
LANES = 128
ROWS_PER_CHUNK = 8
W_CHUNK = 256
W_AHEAD = 16
KV_AHEAD = 12
UP_COLS = 256
AHEAD = 4
OUT_COLS = 512
BLOCK_US = 0.9
F32 = jnp.float32
BF16 = jnp.bfloat16
HBM = pl.BlockSpec(memory_space=pltpu.HBM)
VMEM = pl.BlockSpec(memory_space=pltpu.VMEM)
MESH = pl.DeviceIdType.MESH


def norm_into(x_ref, gamma_ref, beta_ref, dst_ref):
    rows, width = x_ref.shape
    tiles = width // LANES

    def tile(c):
        return x_ref[:, pl.ds(pl.multiple_of(c * LANES, LANES), LANES)].astype(F32)

    zero = jnp.zeros((rows, LANES), F32)
    total = lax.fori_loop(0, tiles, lambda c, s: s + tile(c), zero, unroll=4)
    mean = jnp.sum(total, axis=-1, keepdims=True) / width

    def square(c, s):
        d = tile(c) - mean
        return s + d * d

    var = jnp.sum(lax.fori_loop(0, tiles, square, zero, unroll=4), axis=-1, keepdims=True) / width
    inv = lax.rsqrt(var + LN_EPS)

    def write(c, carry):
        y = (tile(c) - mean) * inv * gamma_ref[pl.ds(c, 1), :] + beta_ref[pl.ds(c, 1), :]
        dst_ref[:, pl.ds(pl.multiple_of(c * LANES, LANES), LANES)] = y.astype(BF16)
        return carry

    lax.fori_loop(0, tiles, write, 0, unroll=4)


def attention_kernel(pos_hbm, pos_row_hbm, x_hbm, gamma_hbm, beta_hbm, w_ref, k_ref, v_ref, ctx_ref, ko_ref, vo_ref,
                     pos_ref, pos_row, x_ref, gamma_ref, beta_ref,
                     wbuf, wf, acc, attn, q_s, kn_s, vn_s, kbuf, vbuf, small, wsem, insem, outsem):
    rows, width = x_ref.shape
    _, groups, slots, head = k_ref.shape
    cols = 3 * groups
    n_w = width // W_CHUNK
    n_c = rows // ROWS_PER_CHUNK
    wrows = W_CHUNK * cols

    def w_copy(c):
        at = pl.ds(pl.multiple_of(c * wrows, wrows), wrows)
        return pltpu.make_async_copy(w_ref.at[at], wbuf.at[at], wsem.at[c])

    def io(i, which, out):
        hbm_in, hbm_out, buf = ((k_ref, ko_ref, kbuf), (v_ref, vo_ref, vbuf))[which]
        at = pl.ds(i * ROWS_PER_CHUNK, ROWS_PER_CHUNK)
        if out:
            return pltpu.make_async_copy(buf.at[at], hbm_out.at[at], outsem.at[which, i])
        return pltpu.make_async_copy(hbm_in.at[at], buf.at[at], insem.at[which, i])

    def kv_start(i):
        io(i, 0, False).start(priority=1)
        io(i, 1, False).start(priority=1)

    first = [pltpu.make_async_copy(src, dst, small.at[n]) for n, (src, dst) in enumerate(
        ((x_hbm, x_ref), (gamma_hbm, gamma_ref), (beta_hbm, beta_ref), (pos_row_hbm, pos_row), (pos_hbm, pos_ref)))]
    for copy in first:
        copy.start()
    for c in range(W_AHEAD):
        w_copy(c).start(priority=1)
    for copy in first:
        copy.wait()

    norm_into(x_ref, gamma_ref, beta_ref, attn)
    acc[...] = jnp.zeros_like(acc)

    def project(c, carry):
        w_copy(c).wait()

        @pl.when(c + W_AHEAD < n_w)
        def _():
            w_copy(c + W_AHEAD).start(priority=1)

        @pl.when(c >= n_w - KV_AHEAD)
        def _():
            kv_start(c - (n_w - KV_AHEAD))

        wf[...] = wbuf[pl.ds(pl.multiple_of(c * wrows, wrows), wrows), :].astype(F32)
        lhs = attn[:, pl.ds(pl.multiple_of(c * W_CHUNK, W_CHUNK), W_CHUNK)]
        for n in range(0, cols, 2):
            rhs = jnp.concatenate(
                [wf[pl.ds(n + e, W_CHUNK, stride=cols), :].astype(BF16) for e in range(2)], axis=1)
            acc[:, n * head:(n + 2) * head] += jnp.dot(lhs, rhs, preferred_element_type=F32)
        return carry

    lax.fori_loop(0, n_w, project, 0)

    lane = lax.broadcasted_iota(jnp.int32, (rows, head), 1)
    freq = jnp.exp(lax.rem(lane, head // 2).astype(F32) * (-2.0 * math.log(ROPE_BASE) / head))
    angle = jnp.broadcast_to(pos_row[...].astype(F32), (rows, rows)).T * freq
    cos_t = jnp.cos(angle)
    sin_t = jnp.where(lane < head // 2, -1.0, 1.0) * jnp.sin(angle)

    def rotate(u):
        u = u.astype(BF16).astype(F32)
        return (u * cos_t + pltpu.roll(u, head // 2, 1) * sin_t).astype(BF16).astype(F32)

    for g in range(groups):
        at = pl.ds(g, rows, stride=groups)
        q_s[at, :] = rotate(acc[:, g * head:(g + 1) * head])
        kn_s[at, :] = rotate(acc[:, (groups + g) * head:(groups + g + 1) * head])
        vn_s[at, :] = acc[:, (2 * groups + g) * head:(2 * groups + g + 1) * head].astype(BF16).astype(F32)

    row16 = lax.broadcasted_iota(jnp.int32, (16, head), 0)
    per_chunk = ROWS_PER_CHUNK * groups
    slot_id = lax.broadcasted_iota(jnp.int32, (slots, per_chunk), 0)
    lane_id = lax.broadcasted_iota(jnp.int32, (slots, per_chunk), 1)
    scale = head ** -0.5

    def chunk(i, carry):
        io(i, 0, False).wait()
        io(i, 1, False).wait()

        @pl.when(i + KV_AHEAD < n_c)
        def _():
            kv_start(i + KV_AHEAD)

        def write_row(r, carry):
            b = i * ROWS_PER_CHUNK + r
            pos = pos_ref[b]
            base = pl.multiple_of((pos // 16) * 16, 16)
            hit = row16 == pos - base
            for g in range(groups):
                for buf, new in ((kbuf, kn_s), (vbuf, vn_s)):
                    old = buf[b, g, pl.ds(base, 16), :].astype(F32)
                    row = new[pl.ds(b * groups + g, 1), :]
                    buf[b, g, pl.ds(base, 16), :] = jnp.where(hit, row, old).astype(BF16)
            return carry

        lax.fori_loop(0, ROWS_PER_CHUNK, write_row, 0, unroll=True)
        io(i, 0, True).start()
        io(i, 1, True).start()

        at = pl.ds(pl.multiple_of(i * per_chunk, per_chunk), per_chunk)
        queries = q_s[at, :].astype(BF16)
        s = jnp.zeros((slots, per_chunk), F32)
        limit = jnp.zeros((slots, per_chunk), jnp.int32)
        for r in range(ROWS_PER_CHUNK):
            b = i * ROWS_PER_CHUNK + r
            every = lax.dot_general(kbuf[b].reshape(groups * slots, head), queries, (((1,), (1,)), ((), ())),
                                    preferred_element_type=F32)
            for g in range(groups):
                s = jnp.where(lane_id == r * groups + g, every[g * slots:(g + 1) * slots], s)
            limit = jnp.where(lane_id >= r * groups, pos_ref[b], limit)
        s = jnp.where(slot_id <= limit, s * scale, NEG_BIG)
        e = jnp.exp(s - jnp.max(s, axis=0, keepdims=True))
        p = (e / jnp.sum(e, axis=0, keepdims=True)).astype(BF16).astype(F32)
        for r in range(ROWS_PER_CHUNK):
            b = i * ROWS_PER_CHUNK + r
            for g in range(groups):
                n = r * groups + g
                weighted = jnp.broadcast_to(p[:, n:n + 1], (slots, head)) * vbuf[b, g].astype(F32)
                ctx_ref[pl.ds(b * groups + g, 1), :] = jnp.sum(weighted, axis=0, keepdims=True).astype(BF16).astype(F32)
        return carry

    lax.fori_loop(0, n_c, chunk, 0)
    for i in range(n_c):
        io(i, 0, True).wait()
        io(i, 1, True).wait()


def attend(x, gamma, beta, w_qkv, k_cache, v_cache, positions):
    rows, width = x.shape
    _, groups, slots, head = k_cache.shape
    cols = 3 * groups
    w_rows = jnp.transpose(w_qkv, (0, 2, 1, 3)).reshape(width * cols, head)
    n_w, n_c = width // W_CHUNK, rows // ROWS_PER_CHUNK
    return pl.pallas_call(
        attention_kernel,
        out_shape=[jax.ShapeDtypeStruct((rows * groups, head), F32),
                   jax.ShapeDtypeStruct(k_cache.shape, k_cache.dtype),
                   jax.ShapeDtypeStruct(v_cache.shape, v_cache.dtype)],
        in_specs=[HBM] * 8,
        out_specs=[VMEM, HBM, HBM],
        scratch_shapes=[
            pltpu.SMEM((rows,), jnp.int32),
            pltpu.VMEM((1, rows), jnp.int32),
            pltpu.VMEM((rows, width), BF16),
            pltpu.VMEM((width // LANES, LANES), F32),
            pltpu.VMEM((width // LANES, LANES), F32),
            pltpu.VMEM((width * cols, head), BF16),
            pltpu.VMEM((W_CHUNK * cols, head), F32),
            pltpu.VMEM((rows, cols * head), F32),
            pltpu.VMEM((rows, width), BF16),
            pltpu.VMEM((rows * groups, head), F32),
            pltpu.VMEM((rows * groups, head), F32),
            pltpu.VMEM((rows * groups, head), F32),
            pltpu.VMEM(k_cache.shape, BF16),
            pltpu.VMEM(v_cache.shape, BF16),
            pltpu.SemaphoreType.DMA((5,)),
            pltpu.SemaphoreType.DMA((n_w,)),
            pltpu.SemaphoreType.DMA((2, n_c)),
            pltpu.SemaphoreType.DMA((2, n_c)),
        ],
        compiler_params=pltpu.CompilerParams(vmem_limit_bytes=53 * 1024 * 1024),
        name='attend',
    )(positions, positions.reshape(1, rows), x, gamma.reshape(-1, LANES), beta.reshape(-1, LANES), w_rows, k_cache, v_cache)


def mlp_kernel(x_hbm, gamma_hbm, beta_hbm, ctx_ref, wo_ref, wu_ref, wd_ref, out_ref,
               x_ref, gamma_ref, beta_ref, small, wub, wcat, mlp_in, lhs, part, d2d_src, d2d_dst, cs32, csb, inbox, outb, usem, dsem, osem, send, recv):
    n_u, _, cu = wub.shape
    n_b, _, cb = wcat.shape
    half, slab = d2d_src.shape[1], inbox.shape[2]
    chips = half // slab
    rows = x_ref.shape[0]
    ctx_width = wo_ref.shape[0]
    groups = ctx_width // LANES
    me = lax.axis_index('tp')
    p, c = lax.div(me, 2), lax.rem(me, 2)
    others = (2, 1, 3)
    partner = me + 1 - 2 * c

    def same_core(q):
        return 2 * lax.rem(p + q, chips) + c

    def up_copy(u):
        return pltpu.make_async_copy(wu_ref.at[:, pl.ds(u * cu, cu)], wub.at[u], usem.at[u])

    def down_copy(j):
        return pltpu.make_async_copy(wd_ref.at[:, pl.ds(j * cb, cb)], wcat.at[j, pl.ds(ctx_width, wd_ref.shape[0])], dsem.at[j])

    def out_copy(j):
        return pltpu.make_async_copy(wo_ref.at[:, pl.ds(j * cb, cb)], wcat.at[j, pl.ds(0, ctx_width)], osem.at[j])

    def fetch(n):
        if n < n_u:
            up_copy(n).start()
        elif n < n_u + n_b:
            out_copy(n - n_u).start()
            down_copy(n - n_u).start()

    first = [pltpu.make_async_copy(src, dst, small.at[n]) for n, (src, dst) in enumerate(
        ((x_hbm, x_ref), (gamma_hbm, gamma_ref), (beta_hbm, beta_ref)))]
    for copy in first:
        copy.start()
    for n in range(AHEAD):
        fetch(n)

    barrier = pltpu.get_barrier_semaphore()
    for peer in tuple(same_core(q) for q in others) + (partner,):
        pl.semaphore_signal(barrier, inc=1, device_id={'tp': peer}, device_id_type=MESH)

    def in_half(q):
        return pl.ds(pl.multiple_of(lax.rem(p + q, chips) * slab, slab), slab)

    def in_rows(q, core):
        return pl.ds(pl.multiple_of(core * half + lax.rem(p + q, chips) * slab, slab), slab)

    def remote(kind, j):
        mine = in_rows(0, c)
        if kind == 0:
            src, dst, peer = d2d_src.at[j], d2d_dst.at[j], partner
        elif kind < 4:
            q = others[kind - 1]
            src, dst, peer = csb.at[j, in_half(q)], inbox.at[j, kind - 1], same_core(q)
        elif kind < 7:
            src, dst, peer = outb.at[j, mine], outb.at[j, mine], same_core(others[kind - 4])
        elif kind == 7:
            src, dst, peer = outb.at[j, mine], outb.at[j, mine], partner
        else:
            far = in_rows(chips - others[kind - 8], c)
            src, dst, peer = outb.at[j, far], outb.at[j, far], partner
        return pltpu.make_async_remote_copy(src_ref=src, dst_ref=dst, send_sem=send.at[kind, j], recv_sem=recv.at[kind, j],
                                            device_id={'tp': peer}, device_id_type=MESH)

    for copy in first:
        copy.wait()
    norm_into(x_ref, gamma_ref, beta_ref, mlp_in)
    for g in range(groups):
        lhs[:, g * LANES:(g + 1) * LANES] = ctx_ref[pl.ds(g, rows, stride=groups), :].astype(BF16)

    for u in range(n_u):
        up_copy(u).wait()
        fetch(u + AHEAD)
        z = jnp.dot(mlp_in[...], wub[u], preferred_element_type=F32)
        at = ctx_width + u * cu
        lhs[:, at:at + cu] = (0.5 * z * (1.0 + lax.erf(z * 0.5 ** 0.5))).astype(BF16)

    pl.semaphore_wait(barrier, 4)

    own_half = pl.ds(pl.multiple_of(c * half, half), half)
    other_half = pl.ds(pl.multiple_of((1 - c) * half, half), half)

    def compute(j):
        out_copy(j).wait()
        down_copy(j).wait()
        fetch(n_u + j + AHEAD)
        part[j] = jnp.dot(lhs[...], wcat[j], preferred_element_type=F32)
        d2d_src[j] = part[j, other_half].astype(BF16)
        remote(0, j).start()

    def chip_sum(j):
        remote(0, j).wait_recv()
        y = part[j, own_half] + d2d_dst[j].astype(F32)
        cs32[j] = y
        csb[j] = y.astype(BF16)
        for kind in (1, 2, 3):
            remote(kind, j).start()

    def finish(j):
        y = cs32[j, in_half(0)]
        for kind in (1, 2, 3):
            remote(kind, j).wait_recv()
            y += inbox[j, kind - 1].astype(F32)
        mine = in_rows(0, c)
        outb[j, mine] = (x_ref[mine, j * cb:(j + 1) * cb].astype(F32) + y).astype(BF16)
        for kind in (4, 5, 6, 7):
            remote(kind, j).start()

    def share(j):
        for kind in (4, 5, 6):
            remote(kind, j).wait_recv()
            remote(kind + 4, j).start()

    def collect(j):
        for kind in (7, 8, 9, 10):
            remote(kind, j).wait_recv()
        out_ref[:, j * cb:(j + 1) * cb] = outb[j]

    stages = ((compute, 0.0), (chip_sum, 1.6), (finish, 5.6), (share, 10.0), (collect, 11.6))
    plan = sorted((j * BLOCK_US + after, n, j) for n, (_, after) in enumerate(stages) for j in range(n_b))
    for _, n, j in plan:
        stages[n][0](j)
    for j in range(n_b):
        for kind in range(11):
            remote(kind, j).wait_send()


def mlp_and_sum(mesh, x, gamma, beta, context, w_out, w_up, w_down):
    rows, width = x.shape
    hidden = w_up.shape[1]
    ctx_width = w_out.shape[0]
    chips = mesh.shape['tp'] // 2
    assert chips == 4
    n_u, n_b = hidden // UP_COLS, width // OUT_COLS
    half, slab = rows // 2, rows // 2 // chips

    def block(dtype, *shape):
        return pltpu.VMEM((n_b,) + shape, dtype)

    return pl.pallas_call(
        mlp_kernel,
        out_shape=jax.ShapeDtypeStruct(x.shape, x.dtype),
        in_specs=[HBM, HBM, HBM, VMEM, HBM, HBM, HBM],
        out_specs=VMEM,
        scratch_shapes=[
            pltpu.VMEM((rows, width), BF16),
            pltpu.VMEM((width // LANES, LANES), F32),
            pltpu.VMEM((width // LANES, LANES), F32),
            pltpu.SemaphoreType.DMA((3,)),
            pltpu.VMEM((n_u, width, UP_COLS), BF16),
            block(BF16, ctx_width + hidden, OUT_COLS),
            pltpu.VMEM((rows, width), BF16),
            pltpu.VMEM((rows, ctx_width + hidden), BF16),
            block(F32, rows, OUT_COLS),
            block(BF16, half, OUT_COLS),
            block(BF16, half, OUT_COLS),
            block(F32, half, OUT_COLS),
            block(BF16, half, OUT_COLS),
            block(BF16, chips - 1, slab, OUT_COLS),
            block(BF16, rows, OUT_COLS),
            pltpu.SemaphoreType.DMA((n_u,)),
            pltpu.SemaphoreType.DMA((n_b,)),
            pltpu.SemaphoreType.DMA((n_b,)),
            pltpu.SemaphoreType.DMA((11, n_b)),
            pltpu.SemaphoreType.DMA((11, n_b)),
        ],
        compiler_params=pltpu.CompilerParams(vmem_limit_bytes=48 * 1024 * 1024, collective_id=0, has_side_effects=True),
        name='mlp_and_sum',
    )(x, gamma.reshape(-1, LANES), beta.reshape(-1, LANES), context, w_out, w_up, w_down)


def solution(mesh):
    row_spec = P('dp', None)
    vec_spec = P(None)
    cache_spec = P('dp', 'tp', None, None)

    def device_step(x, ln_attn_gamma, ln_attn_beta, ln_mlp_gamma, ln_mlp_beta, w_qkv, w_out, w_up, w_down, k_cache, v_cache, positions):
        context, keys_all, values_all = attend(x, ln_attn_gamma, ln_attn_beta, w_qkv, k_cache, v_cache, positions)
        layer_out = mlp_and_sum(mesh, x, ln_mlp_gamma, ln_mlp_beta, context, w_out.reshape(-1, x.shape[1]), w_up, w_down)
        return layer_out, keys_all, values_all

    return jax.shard_map(device_step, mesh=mesh, in_specs=(row_spec, vec_spec, vec_spec, vec_spec, vec_spec, P(None, 'tp', None, None), P('tp', None, None, None), P(None, 'tp'), P('tp', None), cache_spec, cache_spec, P('dp')), out_specs=(row_spec, cache_spec, cache_spec), check_vma=False)
```

```python
import math

import jax
import jax.numpy as jnp
from jax import lax
from jax.experimental import pallas as pl
from jax.experimental.pallas import tpu as pltpu
from jax.sharding import PartitionSpec as P

LN_EPS = 1e-5
ROPE_BASE = 10000.0
NEG_BIG = -1e30
LANES = 128
ROWS_PER_CHUNK = 8
W_CHUNK = 256
W_AHEAD = 16
KV_AHEAD = 12
UP_COLS = 256
AHEAD = 6
OUT_COLS = 512
BLOCK_US = 0.9
F32 = jnp.float32
BF16 = jnp.bfloat16
HBM = pl.BlockSpec(memory_space=pltpu.HBM)
VMEM = pl.BlockSpec(memory_space=pltpu.VMEM)
MESH = pl.DeviceIdType.MESH


def norm_into(x_ref, gamma_ref, beta_ref, dst_ref):
    rows, width = x_ref.shape
    tiles = width // LANES

    def tile(c):
        return x_ref[:, pl.ds(pl.multiple_of(c * LANES, LANES), LANES)].astype(F32)

    zero = jnp.zeros((rows, LANES), F32)
    total = lax.fori_loop(0, tiles, lambda c, s: s + tile(c), zero, unroll=4)
    mean = jnp.sum(total, axis=-1, keepdims=True) / width

    def square(c, s):
        d = tile(c) - mean
        return s + d * d

    var = jnp.sum(lax.fori_loop(0, tiles, square, zero, unroll=4), axis=-1, keepdims=True) / width
    inv = lax.rsqrt(var + LN_EPS)

    def write(c, carry):
        y = (tile(c) - mean) * inv * gamma_ref[pl.ds(c, 1), :] + beta_ref[pl.ds(c, 1), :]
        dst_ref[:, pl.ds(pl.multiple_of(c * LANES, LANES), LANES)] = y.astype(BF16)
        return carry

    lax.fori_loop(0, tiles, write, 0, unroll=4)


def attention_kernel(pos_hbm, pos_row_hbm, x_hbm, gamma_hbm, beta_hbm, w_ref, k_ref, v_ref, ctx_ref, ko_ref, vo_ref,
                     pos_ref, pos_row, x_ref, gamma_ref, beta_ref,
                     wbuf, wf, acc, attn, q_s, kn_s, vn_s, kbuf, vbuf, small, wsem, insem, outsem):
    rows, width = x_ref.shape
    _, groups, slots, head = k_ref.shape
    cols = 3 * groups
    n_w = width // W_CHUNK
    n_c = rows // ROWS_PER_CHUNK
    wrows = W_CHUNK * cols

    def w_copy(c):
        at = pl.ds(pl.multiple_of(c * wrows, wrows), wrows)
        return pltpu.make_async_copy(w_ref.at[at], wbuf.at[at], wsem.at[c])

    def io(i, which, out):
        hbm_in, hbm_out, buf = ((k_ref, ko_ref, kbuf), (v_ref, vo_ref, vbuf))[which]
        at = pl.ds(i * ROWS_PER_CHUNK, ROWS_PER_CHUNK)
        if out:
            return pltpu.make_async_copy(buf.at[at], hbm_out.at[at], outsem.at[which, i])
        return pltpu.make_async_copy(hbm_in.at[at], buf.at[at], insem.at[which, i])

    def kv_start(i):
        io(i, 0, False).start(priority=1)
        io(i, 1, False).start(priority=1)

    first = [pltpu.make_async_copy(src, dst, small.at[n]) for n, (src, dst) in enumerate(
        ((x_hbm, x_ref), (gamma_hbm, gamma_ref), (beta_hbm, beta_ref), (pos_row_hbm, pos_row), (pos_hbm, pos_ref)))]
    for copy in first:
        copy.start()
    for c in range(W_AHEAD):
        w_copy(c).start(priority=1)
    for copy in first:
        copy.wait()

    norm_into(x_ref, gamma_ref, beta_ref, attn)
    acc[...] = jnp.zeros_like(acc)

    def project(c, carry):
        w_copy(c).wait()

        @pl.when(c + W_AHEAD < n_w)
        def _():
            w_copy(c + W_AHEAD).start(priority=1)

        @pl.when(c >= n_w - KV_AHEAD)
        def _():
            kv_start(c - (n_w - KV_AHEAD))

        wf[...] = wbuf[pl.ds(pl.multiple_of(c * wrows, wrows), wrows), :].astype(F32)
        lhs = attn[:, pl.ds(pl.multiple_of(c * W_CHUNK, W_CHUNK), W_CHUNK)]
        for n in range(0, cols, 2):
            rhs = jnp.concatenate(
                [wf[pl.ds(n + e, W_CHUNK, stride=cols), :].astype(BF16) for e in range(2)], axis=1)
            acc[:, n * head:(n + 2) * head] += jnp.dot(lhs, rhs, preferred_element_type=F32)
        return carry

    lax.fori_loop(0, n_w, project, 0)

    lane = lax.broadcasted_iota(jnp.int32, (rows, head), 1)
    freq = jnp.exp(lax.rem(lane, head // 2).astype(F32) * (-2.0 * math.log(ROPE_BASE) / head))
    angle = jnp.broadcast_to(pos_row[...].astype(F32), (rows, rows)).T * freq
    cos_t = jnp.cos(angle)
    sin_t = jnp.where(lane < head // 2, -1.0, 1.0) * jnp.sin(angle)

    def rotate(u):
        u = u.astype(BF16).astype(F32)
        return (u * cos_t + pltpu.roll(u, head // 2, 1) * sin_t).astype(BF16).astype(F32)

    for g in range(groups):
        at = pl.ds(g, rows, stride=groups)
        q_s[at, :] = rotate(acc[:, g * head:(g + 1) * head])
        kn_s[at, :] = rotate(acc[:, (groups + g) * head:(groups + g + 1) * head])
        vn_s[at, :] = acc[:, (2 * groups + g) * head:(2 * groups + g + 1) * head].astype(BF16).astype(F32)

    row16 = lax.broadcasted_iota(jnp.int32, (16, head), 0)
    per_chunk = ROWS_PER_CHUNK * groups
    slot_id = lax.broadcasted_iota(jnp.int32, (slots, per_chunk), 0)
    lane_id = lax.broadcasted_iota(jnp.int32, (slots, per_chunk), 1)
    scale = head ** -0.5

    def chunk(i, carry):
        io(i, 0, False).wait()
        io(i, 1, False).wait()

        @pl.when(i + KV_AHEAD < n_c)
        def _():
            kv_start(i + KV_AHEAD)

        def write_row(r, carry):
            b = i * ROWS_PER_CHUNK + r
            pos = pos_ref[b]
            base = pl.multiple_of((pos // 16) * 16, 16)
            hit = row16 == pos - base
            for g in range(groups):
                for buf, new in ((kbuf, kn_s), (vbuf, vn_s)):
                    old = buf[b, g, pl.ds(base, 16), :].astype(F32)
                    row = new[pl.ds(b * groups + g, 1), :]
                    buf[b, g, pl.ds(base, 16), :] = jnp.where(hit, row, old).astype(BF16)
            return carry

        lax.fori_loop(0, ROWS_PER_CHUNK, write_row, 0, unroll=True)
        io(i, 0, True).start()
        io(i, 1, True).start()

        at = pl.ds(pl.multiple_of(i * per_chunk, per_chunk), per_chunk)
        queries = q_s[at, :].astype(BF16)
        s = jnp.zeros((slots, per_chunk), F32)
        limit = jnp.zeros((slots, per_chunk), jnp.int32)
        for r in range(ROWS_PER_CHUNK):
            b = i * ROWS_PER_CHUNK + r
            every = lax.dot_general(kbuf[b].reshape(groups * slots, head), queries, (((1,), (1,)), ((), ())),
                                    preferred_element_type=F32)
            for g in range(groups):
                s = jnp.where(lane_id == r * groups + g, every[g * slots:(g + 1) * slots], s)
            limit = jnp.where(lane_id >= r * groups, pos_ref[b], limit)
        s = jnp.where(slot_id <= limit, s * scale, NEG_BIG)
        e = jnp.exp(s - jnp.max(s, axis=0, keepdims=True))
        p = (e / jnp.sum(e, axis=0, keepdims=True)).astype(BF16).astype(F32)
        for r in range(ROWS_PER_CHUNK):
            b = i * ROWS_PER_CHUNK + r
            for g in range(groups):
                n = r * groups + g
                weighted = jnp.broadcast_to(p[:, n:n + 1], (slots, head)) * vbuf[b, g].astype(F32)
                ctx_ref[pl.ds(b * groups + g, 1), :] = jnp.sum(weighted, axis=0, keepdims=True).astype(BF16).astype(F32)
        return carry

    lax.fori_loop(0, n_c, chunk, 0)
    for i in range(n_c):
        io(i, 0, True).wait()
        io(i, 1, True).wait()


def attend(x, gamma, beta, w_qkv, k_cache, v_cache, positions):
    rows, width = x.shape
    _, groups, slots, head = k_cache.shape
    cols = 3 * groups
    w_rows = jnp.transpose(w_qkv, (0, 2, 1, 3)).reshape(width * cols, head)
    n_w, n_c = width // W_CHUNK, rows // ROWS_PER_CHUNK
    return pl.pallas_call(
        attention_kernel,
        out_shape=[jax.ShapeDtypeStruct((rows * groups, head), F32),
                   jax.ShapeDtypeStruct(k_cache.shape, k_cache.dtype),
                   jax.ShapeDtypeStruct(v_cache.shape, v_cache.dtype)],
        in_specs=[HBM] * 8,
        out_specs=[VMEM, HBM, HBM],
        scratch_shapes=[
            pltpu.SMEM((rows,), jnp.int32),
            pltpu.VMEM((1, rows), jnp.int32),
            pltpu.VMEM((rows, width), BF16),
            pltpu.VMEM((width // LANES, LANES), F32),
            pltpu.VMEM((width // LANES, LANES), F32),
            pltpu.VMEM((width * cols, head), BF16),
            pltpu.VMEM((W_CHUNK * cols, head), F32),
            pltpu.VMEM((rows, cols * head), F32),
            pltpu.VMEM((rows, width), BF16),
            pltpu.VMEM((rows * groups, head), F32),
            pltpu.VMEM((rows * groups, head), F32),
            pltpu.VMEM((rows * groups, head), F32),
            pltpu.VMEM(k_cache.shape, BF16),
            pltpu.VMEM(v_cache.shape, BF16),
            pltpu.SemaphoreType.DMA((5,)),
            pltpu.SemaphoreType.DMA((n_w,)),
            pltpu.SemaphoreType.DMA((2, n_c)),
            pltpu.SemaphoreType.DMA((2, n_c)),
        ],
        compiler_params=pltpu.CompilerParams(vmem_limit_bytes=53 * 1024 * 1024),
        name='attend',
    )(*(pltpu.with_memory_space_constraint(a, pltpu.HBM) for a in (
        positions, positions.reshape(1, rows), x, gamma.reshape(-1, LANES), beta.reshape(-1, LANES))), w_rows, k_cache, v_cache)


def mlp_kernel(x_hbm, gamma_hbm, beta_hbm, ctx_ref, wo_ref, wu_ref, wd_ref, out_ref,
               x_ref, gamma_ref, beta_ref, small, wub, wcat, mlp_in, lhs, part, d2d_src, d2d_dst, cs32, csb, inbox, outb, usem, dsem, osem, send, recv):
    n_u, _, cu = wub.shape
    n_b, _, cb = wcat.shape
    half, slab = d2d_src.shape[1], inbox.shape[2]
    chips = half // slab
    rows = x_ref.shape[0]
    ctx_width = wo_ref.shape[0]
    groups = ctx_width // LANES
    me = lax.axis_index('tp')
    p, c = lax.div(me, 2), lax.rem(me, 2)
    others = (2, 1, 3)
    partner = me + 1 - 2 * c

    def same_core(q):
        return 2 * lax.rem(p + q, chips) + c

    def up_copy(u):
        return pltpu.make_async_copy(wu_ref.at[:, pl.ds(u * cu, cu)], wub.at[u], usem.at[u])

    def down_copy(j):
        return pltpu.make_async_copy(wd_ref.at[:, pl.ds(j * cb, cb)], wcat.at[j, pl.ds(ctx_width, wd_ref.shape[0])], dsem.at[j])

    def out_copy(j):
        return pltpu.make_async_copy(wo_ref.at[:, pl.ds(j * cb, cb)], wcat.at[j, pl.ds(0, ctx_width)], osem.at[j])

    def fetch(n):
        if n < n_u:
            up_copy(n).start()
        elif n < n_u + n_b:
            out_copy(n - n_u).start()
            down_copy(n - n_u).start()

    first = [pltpu.make_async_copy(src, dst, small.at[n]) for n, (src, dst) in enumerate(
        ((x_hbm, x_ref), (gamma_hbm, gamma_ref), (beta_hbm, beta_ref)))]
    for copy in first:
        copy.start()
    for n in range(AHEAD):
        fetch(n)

    barrier = pltpu.get_barrier_semaphore()
    for peer in tuple(same_core(q) for q in others) + (partner,):
        pl.semaphore_signal(barrier, inc=1, device_id={'tp': peer}, device_id_type=MESH)

    def in_half(q):
        return pl.ds(pl.multiple_of(lax.rem(p + q, chips) * slab, slab), slab)

    def in_rows(q, core):
        return pl.ds(pl.multiple_of(core * half + lax.rem(p + q, chips) * slab, slab), slab)

    def remote(kind, j):
        mine = in_rows(0, c)
        if kind == 0:
            src, dst, peer = d2d_src.at[j], d2d_dst.at[j], partner
        elif kind < 4:
            q = others[kind - 1]
            src, dst, peer = csb.at[j, in_half(q)], inbox.at[j, kind - 1], same_core(q)
        elif kind < 7:
            src, dst, peer = outb.at[j, mine], outb.at[j, mine], same_core(others[kind - 4])
        elif kind == 7:
            src, dst, peer = outb.at[j, mine], outb.at[j, mine], partner
        else:
            far = in_rows(chips - others[kind - 8], c)
            src, dst, peer = outb.at[j, far], outb.at[j, far], partner
        return pltpu.make_async_remote_copy(src_ref=src, dst_ref=dst, send_sem=send.at[kind, j], recv_sem=recv.at[kind, j],
                                            device_id={'tp': peer}, device_id_type=MESH)

    for copy in first:
        copy.wait()
    norm_into(x_ref, gamma_ref, beta_ref, mlp_in)
    for g in range(groups):
        lhs[:, g * LANES:(g + 1) * LANES] = ctx_ref[pl.ds(g, rows, stride=groups), :].astype(BF16)

    for u in range(n_u):
        up_copy(u).wait()
        fetch(u + AHEAD)
        z = jnp.dot(mlp_in[...], wub[u], preferred_element_type=F32)
        at = ctx_width + u * cu
        lhs[:, at:at + cu] = (0.5 * z * (1.0 + lax.erf(z * 0.5 ** 0.5))).astype(BF16)

    pl.semaphore_wait(barrier, 4)

    own_half = pl.ds(pl.multiple_of(c * half, half), half)
    other_half = pl.ds(pl.multiple_of((1 - c) * half, half), half)

    def compute(j):
        out_copy(j).wait()
        down_copy(j).wait()
        fetch(n_u + j + AHEAD)
        part[j] = jnp.dot(lhs[...], wcat[j], preferred_element_type=F32)
        d2d_src[j] = part[j, other_half].astype(BF16)
        remote(0, j).start()

    def chip_sum(j):
        remote(0, j).wait_recv()
        y = part[j, own_half] + d2d_dst[j].astype(F32)
        cs32[j] = y
        csb[j] = y.astype(BF16)
        for kind in (1, 2, 3):
            remote(kind, j).start()

    def finish(j):
        y = cs32[j, in_half(0)]
        for kind in (1, 2, 3):
            remote(kind, j).wait_recv()
            y += inbox[j, kind - 1].astype(F32)
        mine = in_rows(0, c)
        outb[j, mine] = (x_ref[mine, j * cb:(j + 1) * cb].astype(F32) + y).astype(BF16)
        for kind in (4, 5, 6, 7):
            remote(kind, j).start()

    def share(j):
        for kind in (4, 5, 6):
            remote(kind, j).wait_recv()
            remote(kind + 4, j).start()

    def collect(j):
        for kind in (7, 8, 9, 10):
            remote(kind, j).wait_recv()
        out_ref[:, j * cb:(j + 1) * cb] = outb[j]

    stages = ((compute, 0.0), (chip_sum, 1.6), (finish, 6.4), (share, 11.2), (collect, 12.8))
    plan = sorted((j * BLOCK_US + after, n, j) for n, (_, after) in enumerate(stages) for j in range(n_b))
    for _, n, j in plan:
        stages[n][0](j)
    for j in range(n_b):
        for kind in range(11):
            remote(kind, j).wait_send()


def mlp_and_sum(mesh, x, gamma, beta, context, w_out, w_up, w_down):
    rows, width = x.shape
    hidden = w_up.shape[1]
    ctx_width = w_out.shape[0]
    chips = mesh.shape['tp'] // 2
    assert chips == 4
    n_u, n_b = hidden // UP_COLS, width // OUT_COLS
    half, slab = rows // 2, rows // 2 // chips

    def block(dtype, *shape):
        return pltpu.VMEM((n_b,) + shape, dtype)

    return pl.pallas_call(
        mlp_kernel,
        out_shape=jax.ShapeDtypeStruct(x.shape, x.dtype),
        in_specs=[HBM, HBM, HBM, VMEM, HBM, HBM, HBM],
        out_specs=VMEM,
        scratch_shapes=[
            pltpu.VMEM((rows, width), BF16),
            pltpu.VMEM((width // LANES, LANES), F32),
            pltpu.VMEM((width // LANES, LANES), F32),
            pltpu.SemaphoreType.DMA((3,)),
            pltpu.VMEM((n_u, width, UP_COLS), BF16),
            block(BF16, ctx_width + hidden, OUT_COLS),
            pltpu.VMEM((rows, width), BF16),
            pltpu.VMEM((rows, ctx_width + hidden), BF16),
            block(F32, rows, OUT_COLS),
            block(BF16, half, OUT_COLS),
            block(BF16, half, OUT_COLS),
            block(F32, half, OUT_COLS),
            block(BF16, half, OUT_COLS),
            block(BF16, chips - 1, slab, OUT_COLS),
            block(BF16, rows, OUT_COLS),
            pltpu.SemaphoreType.DMA((n_u,)),
            pltpu.SemaphoreType.DMA((n_b,)),
            pltpu.SemaphoreType.DMA((n_b,)),
            pltpu.SemaphoreType.DMA((11, n_b)),
            pltpu.SemaphoreType.DMA((11, n_b)),
        ],
        compiler_params=pltpu.CompilerParams(vmem_limit_bytes=48 * 1024 * 1024, collective_id=0, has_side_effects=True),
        name='mlp_and_sum',
    )(x, gamma.reshape(-1, LANES), beta.reshape(-1, LANES), context, w_out, w_up, w_down)


def solution(mesh):
    row_spec = P('dp', None)
    vec_spec = P(None)
    cache_spec = P('dp', 'tp', None, None)

    def device_step(x, ln_attn_gamma, ln_attn_beta, ln_mlp_gamma, ln_mlp_beta, w_qkv, w_out, w_up, w_down, k_cache, v_cache, positions):
        context, keys_all, values_all = attend(x, ln_attn_gamma, ln_attn_beta, w_qkv, k_cache, v_cache, positions)
        layer_out = mlp_and_sum(mesh, x, ln_mlp_gamma, ln_mlp_beta, context, w_out.reshape(-1, x.shape[1]), w_up, w_down)
        return layer_out, keys_all, values_all

    return jax.shard_map(device_step, mesh=mesh, in_specs=(row_spec, vec_spec, vec_spec, vec_spec, vec_spec, P(None, 'tp', None, None), P('tp', None, None, None), P(None, 'tp'), P('tp', None), cache_spec, cache_spec, P('dp')), out_specs=(row_spec, cache_spec, cache_spec), check_vma=False)
```

```python
import math

import jax
import jax.numpy as jnp
from jax import lax
from jax.experimental import pallas as pl
from jax.experimental.pallas import tpu as pltpu
from jax.sharding import PartitionSpec as P

LN_EPS = 1e-5
ROPE_BASE = 10000.0
NEG_BIG = -1e30
LANES = 128
ROWS_PER_CHUNK = 8
W_CHUNK = 256
W_AHEAD = 16
KV_AHEAD = 12
UP_COLS = 256
AHEAD = 6
OUT_COLS = 512
BLOCK_US = 0.9
F32 = jnp.float32
BF16 = jnp.bfloat16
HBM = pl.BlockSpec(memory_space=pltpu.HBM)
VMEM = pl.BlockSpec(memory_space=pltpu.VMEM)
MESH = pl.DeviceIdType.MESH


def norm_into(x_ref, gamma_ref, beta_ref, dst_ref):
    rows, width = x_ref.shape
    tiles = width // LANES

    def tile(c):
        return x_ref[:, pl.ds(pl.multiple_of(c * LANES, LANES), LANES)].astype(F32)

    zero = jnp.zeros((rows, LANES), F32)
    total = lax.fori_loop(0, tiles, lambda c, s: s + tile(c), zero, unroll=4)
    mean = jnp.sum(total, axis=-1, keepdims=True) / width

    def square(c, s):
        d = tile(c) - mean
        return s + d * d

    var = jnp.sum(lax.fori_loop(0, tiles, square, zero, unroll=4), axis=-1, keepdims=True) / width
    inv = lax.rsqrt(var + LN_EPS)

    def write(c, carry):
        y = (tile(c) - mean) * inv * gamma_ref[pl.ds(c, 1), :] + beta_ref[pl.ds(c, 1), :]
        dst_ref[:, pl.ds(pl.multiple_of(c * LANES, LANES), LANES)] = y.astype(BF16)
        return carry

    lax.fori_loop(0, tiles, write, 0, unroll=4)


def attention_kernel(pos_hbm, pos_row_hbm, x_hbm, gamma_hbm, beta_hbm, w_ref, k_ref, v_ref, ctx_ref, ko_ref, vo_ref,
                     pos_ref, pos_row, x_ref, gamma_ref, beta_ref,
                     wbuf, wf, acc, attn, q_s, kn_s, vn_s, kbuf, vbuf, small, wsem, insem, outsem):
    rows, width = x_ref.shape
    _, groups, slots, head = k_ref.shape
    cols = 3 * groups
    n_w = width // W_CHUNK
    n_c = rows // ROWS_PER_CHUNK
    wrows = W_CHUNK * cols

    def w_copy(c):
        at = pl.ds(pl.multiple_of(c * wrows, wrows), wrows)
        return pltpu.make_async_copy(w_ref.at[at], wbuf.at[at], wsem.at[c])

    def io(i, which, out):
        hbm_in, hbm_out, buf = ((k_ref, ko_ref, kbuf), (v_ref, vo_ref, vbuf))[which]
        at = pl.ds(i * ROWS_PER_CHUNK, ROWS_PER_CHUNK)
        if out:
            return pltpu.make_async_copy(buf.at[at], hbm_out.at[at], outsem.at[which, i])
        return pltpu.make_async_copy(hbm_in.at[at], buf.at[at], insem.at[which, i])

    def kv_start(i):
        io(i, 0, False).start(priority=1)
        io(i, 1, False).start(priority=1)

    first = [pltpu.make_async_copy(src, dst, small.at[n]) for n, (src, dst) in enumerate(
        ((x_hbm, x_ref), (gamma_hbm, gamma_ref), (beta_hbm, beta_ref), (pos_row_hbm, pos_row), (pos_hbm, pos_ref)))]
    for copy in first:
        copy.start()
    for c in range(W_AHEAD):
        w_copy(c).start(priority=1)
    for copy in first:
        copy.wait()

    norm_into(x_ref, gamma_ref, beta_ref, attn)
    acc[...] = jnp.zeros_like(acc)

    def project(c, carry):
        w_copy(c).wait()

        @pl.when(c + W_AHEAD < n_w)
        def _():
            w_copy(c + W_AHEAD).start(priority=1)

        @pl.when(c >= n_w - KV_AHEAD)
        def _():
            kv_start(c - (n_w - KV_AHEAD))

        wf[...] = wbuf[pl.ds(pl.multiple_of(c * wrows, wrows), wrows), :].astype(F32)
        lhs = attn[:, pl.ds(pl.multiple_of(c * W_CHUNK, W_CHUNK), W_CHUNK)]
        for n in range(0, cols, 2):
            rhs = jnp.concatenate(
                [wf[pl.ds(n + e, W_CHUNK, stride=cols), :].astype(BF16) for e in range(2)], axis=1)
            acc[:, n * head:(n + 2) * head] += jnp.dot(lhs, rhs, preferred_element_type=F32)
        return carry

    lax.fori_loop(0, n_w, project, 0)

    lane = lax.broadcasted_iota(jnp.int32, (rows, head), 1)
    freq = jnp.exp(lax.rem(lane, head // 2).astype(F32) * (-2.0 * math.log(ROPE_BASE) / head))
    angle = jnp.broadcast_to(pos_row[...].astype(F32), (rows, rows)).T * freq
    cos_t = jnp.cos(angle)
    sin_t = jnp.where(lane < head // 2, -1.0, 1.0) * jnp.sin(angle)

    def rotate(u):
        u = u.astype(BF16).astype(F32)
        return (u * cos_t + pltpu.roll(u, head // 2, 1) * sin_t).astype(BF16).astype(F32)

    for g in range(groups):
        at = pl.ds(g, rows, stride=groups)
        q_s[at, :] = rotate(acc[:, g * head:(g + 1) * head])
        kn_s[at, :] = rotate(acc[:, (groups + g) * head:(groups + g + 1) * head])
        vn_s[at, :] = acc[:, (2 * groups + g) * head:(2 * groups + g + 1) * head].astype(BF16).astype(F32)

    row16 = lax.broadcasted_iota(jnp.int32, (16, head), 0)
    per_chunk = ROWS_PER_CHUNK * groups
    slot_id = lax.broadcasted_iota(jnp.int32, (slots, per_chunk), 0)
    lane_id = lax.broadcasted_iota(jnp.int32, (slots, per_chunk), 1)
    scale = head ** -0.5

    def chunk(i, carry):
        io(i, 0, False).wait()
        io(i, 1, False).wait()

        @pl.when(i + KV_AHEAD < n_c)
        def _():
            kv_start(i + KV_AHEAD)

        def write_row(r, carry):
            b = i * ROWS_PER_CHUNK + r
            pos = pos_ref[b]
            base = pl.multiple_of((pos // 16) * 16, 16)
            hit = row16 == pos - base
            for g in range(groups):
                for buf, new in ((kbuf, kn_s), (vbuf, vn_s)):
                    old = buf[b, g, pl.ds(base, 16), :].astype(F32)
                    row = new[pl.ds(b * groups + g, 1), :]
                    buf[b, g, pl.ds(base, 16), :] = jnp.where(hit, row, old).astype(BF16)
            return carry

        lax.fori_loop(0, ROWS_PER_CHUNK, write_row, 0, unroll=True)
        io(i, 0, True).start()
        io(i, 1, True).start()

        at = pl.ds(pl.multiple_of(i * per_chunk, per_chunk), per_chunk)
        queries = q_s[at, :].astype(BF16)
        s = jnp.zeros((slots, per_chunk), F32)
        limit = jnp.zeros((slots, per_chunk), jnp.int32)
        for r in range(ROWS_PER_CHUNK):
            b = i * ROWS_PER_CHUNK + r
            every = lax.dot_general(kbuf[b].reshape(groups * slots, head), queries, (((1,), (1,)), ((), ())),
                                    preferred_element_type=F32)
            for g in range(groups):
                s = jnp.where(lane_id == r * groups + g, every[g * slots:(g + 1) * slots], s)
            limit = jnp.where(lane_id >= r * groups, pos_ref[b], limit)
        s = jnp.where(slot_id <= limit, s * scale, NEG_BIG)
        e = jnp.exp(s - jnp.max(s, axis=0, keepdims=True))
        p = (e / jnp.sum(e, axis=0, keepdims=True)).astype(BF16).astype(F32)
        for r in range(ROWS_PER_CHUNK):
            b = i * ROWS_PER_CHUNK + r
            for g in range(groups):
                n = r * groups + g
                weighted = jnp.broadcast_to(p[:, n:n + 1], (slots, head)) * vbuf[b, g].astype(F32)
                ctx_ref[pl.ds(b * groups + g, 1), :] = jnp.sum(weighted, axis=0, keepdims=True).astype(BF16).astype(F32)
        return carry

    lax.fori_loop(0, n_c, chunk, 0)
    for i in range(n_c):
        io(i, 0, True).wait()
        io(i, 1, True).wait()


def attend(x, gamma, beta, w_qkv, k_cache, v_cache, positions):
    rows, width = x.shape
    _, groups, slots, head = k_cache.shape
    cols = 3 * groups
    w_rows = jnp.transpose(w_qkv, (0, 2, 1, 3)).reshape(width * cols, head)
    n_w, n_c = width // W_CHUNK, rows // ROWS_PER_CHUNK
    return pl.pallas_call(
        attention_kernel,
        out_shape=[jax.ShapeDtypeStruct((rows * groups, head), F32),
                   jax.ShapeDtypeStruct(k_cache.shape, k_cache.dtype),
                   jax.ShapeDtypeStruct(v_cache.shape, v_cache.dtype)],
        in_specs=[HBM] * 8,
        out_specs=[VMEM, HBM, HBM],
        scratch_shapes=[
            pltpu.SMEM((rows,), jnp.int32),
            pltpu.VMEM((1, rows), jnp.int32),
            pltpu.VMEM((rows, width), BF16),
            pltpu.VMEM((width // LANES, LANES), F32),
            pltpu.VMEM((width // LANES, LANES), F32),
            pltpu.VMEM((width * cols, head), BF16),
            pltpu.VMEM((W_CHUNK * cols, head), F32),
            pltpu.VMEM((rows, cols * head), F32),
            pltpu.VMEM((rows, width), BF16),
            pltpu.VMEM((rows * groups, head), F32),
            pltpu.VMEM((rows * groups, head), F32),
            pltpu.VMEM((rows * groups, head), F32),
            pltpu.VMEM(k_cache.shape, BF16),
            pltpu.VMEM(v_cache.shape, BF16),
            pltpu.SemaphoreType.DMA((5,)),
            pltpu.SemaphoreType.DMA((n_w,)),
            pltpu.SemaphoreType.DMA((2, n_c)),
            pltpu.SemaphoreType.DMA((2, n_c)),
        ],
        compiler_params=pltpu.CompilerParams(vmem_limit_bytes=53 * 1024 * 1024),
        name='attend',
    )(*(pltpu.with_memory_space_constraint(a, pltpu.HBM) for a in (
        positions, positions.reshape(1, rows), x, gamma.reshape(-1, LANES), beta.reshape(-1, LANES))), w_rows, k_cache, v_cache)


def mlp_kernel(x_hbm, gamma_hbm, beta_hbm, ctx_ref, wo_ref, wu_ref, wd_ref, out_ref,
               x_ref, gamma_ref, beta_ref, small, wub, wcat, mlp_in, lhs, part, d2d_src, d2d_dst, cs32, csb, inbox, outb, usem, dsem, osem, send, recv):
    n_u, _, cu = wub.shape
    n_b, _, cb = wcat.shape
    half, slab = d2d_src.shape[1], inbox.shape[2]
    chips = half // slab
    rows = x_ref.shape[0]
    ctx_width = wo_ref.shape[0]
    groups = ctx_width // LANES
    me = lax.axis_index('tp')
    p, c = lax.div(me, 2), lax.rem(me, 2)
    others = (2, 1, 3)
    partner = me + 1 - 2 * c

    def same_core(q):
        return 2 * lax.rem(p + q, chips) + c

    def up_copy(u):
        return pltpu.make_async_copy(wu_ref.at[:, pl.ds(u * cu, cu)], wub.at[u], usem.at[u])

    def down_copy(j):
        return pltpu.make_async_copy(wd_ref.at[:, pl.ds(j * cb, cb)], wcat.at[j, pl.ds(ctx_width, wd_ref.shape[0])], dsem.at[j])

    def out_copy(j):
        return pltpu.make_async_copy(wo_ref.at[:, pl.ds(j * cb, cb)], wcat.at[j, pl.ds(0, ctx_width)], osem.at[j])

    def fetch(n):
        if n < n_u:
            up_copy(n).start()
        elif n < n_u + n_b:
            out_copy(n - n_u).start()
            down_copy(n - n_u).start()

    first = [pltpu.make_async_copy(src, dst, small.at[n]) for n, (src, dst) in enumerate(
        ((x_hbm, x_ref), (gamma_hbm, gamma_ref), (beta_hbm, beta_ref)))]
    for copy in first:
        copy.start()
    for n in range(AHEAD):
        fetch(n)

    barrier = pltpu.get_barrier_semaphore()
    for peer in tuple(same_core(q) for q in others) + (partner,):
        pl.semaphore_signal(barrier, inc=1, device_id={'tp': peer}, device_id_type=MESH)

    def in_half(q):
        return pl.ds(pl.multiple_of(lax.rem(p + q, chips) * slab, slab), slab)

    def in_rows(q, core):
        return pl.ds(pl.multiple_of(core * half + lax.rem(p + q, chips) * slab, slab), slab)

    def remote(kind, j):
        mine = in_rows(0, c)
        if kind == 0:
            src, dst, peer = d2d_src.at[j], d2d_dst.at[j], partner
        elif kind < 4:
            q = others[kind - 1]
            src, dst, peer = csb.at[j, in_half(q)], inbox.at[j, kind - 1], same_core(q)
        elif kind < 7:
            src, dst, peer = outb.at[j, mine], outb.at[j, mine], same_core(others[kind - 4])
        elif kind == 7:
            src, dst, peer = outb.at[j, mine], outb.at[j, mine], partner
        else:
            far = in_rows(chips - others[kind - 8], c)
            src, dst, peer = outb.at[j, far], outb.at[j, far], partner
        return pltpu.make_async_remote_copy(src_ref=src, dst_ref=dst, send_sem=send.at[kind, j], recv_sem=recv.at[kind, j],
                                            device_id={'tp': peer}, device_id_type=MESH)

    for copy in first:
        copy.wait()
    norm_into(x_ref, gamma_ref, beta_ref, mlp_in)
    for g in range(groups):
        lhs[:, g * LANES:(g + 1) * LANES] = ctx_ref[pl.ds(g, rows, stride=groups), :].astype(BF16)

    for u in range(n_u):
        up_copy(u).wait()
        fetch(u + AHEAD)
        z = jnp.dot(mlp_in[...], wub[u], preferred_element_type=F32)
        at = ctx_width + u * cu
        lhs[:, at:at + cu] = (0.5 * z * (1.0 + lax.erf(z * 0.5 ** 0.5))).astype(BF16)

    pl.semaphore_wait(barrier, 4)

    own_half = pl.ds(pl.multiple_of(c * half, half), half)
    other_half = pl.ds(pl.multiple_of((1 - c) * half, half), half)

    def compute(j):
        out_copy(j).wait()
        down_copy(j).wait()
        fetch(n_u + j + AHEAD)
        part[j] = jnp.dot(lhs[...], wcat[j], preferred_element_type=F32)
        d2d_src[j] = part[j, other_half].astype(BF16)
        remote(0, j).start()

    def chip_sum(j):
        remote(0, j).wait_recv()
        y = part[j, own_half] + d2d_dst[j].astype(F32)
        cs32[j] = y
        csb[j] = y.astype(BF16)
        for kind in (1, 2, 3):
            remote(kind, j).start()

    def finish(j):
        y = cs32[j, in_half(0)]
        for kind in (1, 2, 3):
            remote(kind, j).wait_recv()
            y += inbox[j, kind - 1].astype(F32)
        mine = in_rows(0, c)
        outb[j, mine] = (x_ref[mine, j * cb:(j + 1) * cb].astype(F32) + y).astype(BF16)
        for kind in (4, 5, 6, 7):
            remote(kind, j).start()

    def share(j):
        for kind in (4, 5, 6):
            remote(kind, j).wait_recv()
            remote(kind + 4, j).start()

    def collect(j):
        for kind in (7, 8, 9, 10):
            remote(kind, j).wait_recv()
        out_ref[:, j * cb:(j + 1) * cb] = outb[j]

    stages = ((compute, 0.0), (chip_sum, 1.3), (finish, 4.2), (share, 7.8), (collect, 9.0))
    plan = sorted((j * BLOCK_US + after, n, j) for n, (_, after) in enumerate(stages) for j in range(n_b))
    for _, n, j in plan:
        stages[n][0](j)
    for j in range(n_b):
        for kind in range(11):
            remote(kind, j).wait_send()


def mlp_and_sum(mesh, x, gamma, beta, context, w_out, w_up, w_down):
    rows, width = x.shape
    hidden = w_up.shape[1]
    ctx_width = w_out.shape[0]
    chips = mesh.shape['tp'] // 2
    assert chips == 4
    n_u, n_b = hidden // UP_COLS, width // OUT_COLS
    half, slab = rows // 2, rows // 2 // chips

    def block(dtype, *shape):
        return pltpu.VMEM((n_b,) + shape, dtype)

    return pl.pallas_call(
        mlp_kernel,
        out_shape=jax.ShapeDtypeStruct(x.shape, x.dtype),
        in_specs=[HBM, HBM, HBM, VMEM, HBM, HBM, HBM],
        out_specs=VMEM,
        scratch_shapes=[
            pltpu.VMEM((rows, width), BF16),
            pltpu.VMEM((width // LANES, LANES), F32),
            pltpu.VMEM((width // LANES, LANES), F32),
            pltpu.SemaphoreType.DMA((3,)),
            pltpu.VMEM((n_u, width, UP_COLS), BF16),
            block(BF16, ctx_width + hidden, OUT_COLS),
            pltpu.VMEM((rows, width), BF16),
            pltpu.VMEM((rows, ctx_width + hidden), BF16),
            block(F32, rows, OUT_COLS),
            block(BF16, half, OUT_COLS),
            block(BF16, half, OUT_COLS),
            block(F32, half, OUT_COLS),
            block(BF16, half, OUT_COLS),
            block(BF16, chips - 1, slab, OUT_COLS),
            block(BF16, rows, OUT_COLS),
            pltpu.SemaphoreType.DMA((n_u,)),
            pltpu.SemaphoreType.DMA((n_b,)),
            pltpu.SemaphoreType.DMA((n_b,)),
            pltpu.SemaphoreType.DMA((11, n_b)),
            pltpu.SemaphoreType.DMA((11, n_b)),
        ],
        compiler_params=pltpu.CompilerParams(vmem_limit_bytes=48 * 1024 * 1024, collective_id=0, has_side_effects=True),
        name='mlp_and_sum',
    )(x, gamma.reshape(-1, LANES), beta.reshape(-1, LANES), context, w_out, w_up, w_down)


def solution(mesh):
    row_spec = P('dp', None)
    vec_spec = P(None)
    cache_spec = P('dp', 'tp', None, None)

    def device_step(x, ln_attn_gamma, ln_attn_beta, ln_mlp_gamma, ln_mlp_beta, w_qkv, w_out, w_up, w_down, k_cache, v_cache, positions):
        context, keys_all, values_all = attend(x, ln_attn_gamma, ln_attn_beta, w_qkv, k_cache, v_cache, positions)
        layer_out = mlp_and_sum(mesh, x, ln_mlp_gamma, ln_mlp_beta, context, w_out.reshape(-1, x.shape[1]), w_up, w_down)
        return layer_out, keys_all, values_all

    return jax.shard_map(device_step, mesh=mesh, in_specs=(row_spec, vec_spec, vec_spec, vec_spec, vec_spec, P(None, 'tp', None, None), P('tp', None, None, None), P(None, 'tp'), P('tp', None), cache_spec, cache_spec, P('dp')), out_specs=(row_spec, cache_spec, cache_spec), check_vma=False)
```
